8 devices in a mesh: data: 2 (over z, y), pipe: 4 (over x, core).
Axes of the slice: x: 2, y: 2, z: 1, core: 2. Of those that a mesh axis runs over, the one named last changes fastest.
Arguments:
- x_slice: bfloat16 [4096, 2048], P(('data', 'pipe')), parts along dimension 0
- slice_idx: int32 [8], P(('data', 'pipe')), parts along dimension 0
- k_cache: bfloat16 [28672, 16, 128], P(('data', 'pipe')), parts along dimension 0
- v_cache: bfloat16 [28672, 16, 128], P(('data', 'pipe')), parts along dimension 0
- w_q: bfloat16 [4, 2048, 2048], P('pipe')
- w_kv: bfloat16 [4, 2048, 4096], P('pipe')
- w_o: bfloat16 [4, 2048, 2048], P('pipe')
- w_gate: bfloat16 [4, 2048, 8192], P('pipe')
- w_up: bfloat16 [4, 2048, 8192], P('pipe')
- w_down: bfloat16 [4, 8192, 2048], P('pipe')
Outputs:
- output 1: bfloat16 [4096, 2048], P(('data', 'pipe')), parts along dimension 0
- output 2: float32 [4096, 16], P(('data', 'pipe')), parts along dimension 0
There are 2 independent parts. The reference program is written for one: setup_inputs(seed, part) draws one part's arguments, and reference() takes and returns one part's arrays. A program takes and returns all parts, laid end to end along the dimension named above; an argument that names none is the same for every part.
All inputs are finite; a program needn't handle non-finite values.
Results may differ from the reference program's by a relative error of at most 0.00938952.
Values are sent between devices in bfloat16 or wider.
A program may use at most 1 GiB of HBM per device.

```python
import jax
import jax.numpy as jnp
from jax import lax

STAGES = 4
D_MODEL = 2048
N_HEADS = 16
HEAD_DIM = 128
D_FF = 8192
SLICE_LEN = 512
N_SLICES = 8
P_MAX = 3584
QKV_WIDTH = N_HEADS * HEAD_DIM


def setup_inputs(seed: int = 0, part: int = 0) -> dict:
    shared = jax.random.split(jax.random.key(seed), 8)
    part_keys = jax.random.split(jax.random.fold_in(shared[6], part), 4)
    tick_base = jax.random.randint(shared[7], (), 0, N_SLICES)
    tick_num = (tick_base + part) % N_SLICES
    slice_idx = ((tick_num - jnp.arange(STAGES)) % N_SLICES).astype(jnp.int32)

    def normal_draw(rng_key, dims_shape, spread):
        return (jax.random.normal(rng_key, dims_shape, jnp.float32) * spread).astype(jnp.bfloat16)

    return {
        'x_slice': normal_draw(part_keys[1], (STAGES * SLICE_LEN, D_MODEL), 1.0),
        'slice_idx': slice_idx,
        'k_cache': normal_draw(part_keys[2], (STAGES * P_MAX, N_HEADS, HEAD_DIM), 1.0),
        'v_cache': normal_draw(part_keys[3], (STAGES * P_MAX, N_HEADS, HEAD_DIM), 1.0),
        'w_q': normal_draw(shared[0], (STAGES, D_MODEL, QKV_WIDTH), 2.0 * D_MODEL ** -0.5),
        'w_kv': normal_draw(shared[1], (STAGES, D_MODEL, 2 * QKV_WIDTH), D_MODEL ** -0.5),
        'w_o': normal_draw(shared[2], (STAGES, QKV_WIDTH, D_MODEL), 2.0 * QKV_WIDTH ** -0.5),
        'w_gate': normal_draw(shared[3], (STAGES, D_MODEL, D_FF), D_MODEL ** -0.5),
        'w_up': normal_draw(shared[4], (STAGES, D_MODEL, D_FF), D_MODEL ** -0.5),
        'w_down': normal_draw(shared[5], (STAGES, D_FF, D_MODEL), D_FF ** -0.5),
    }


def rms_normalize(values):
    stats_f32 = values.astype(jnp.float32)
    inv_rms = lax.rsqrt(jnp.mean(stats_f32 * stats_f32, axis=-1, keepdims=True) + 1e-6)
    return (stats_f32 * inv_rms).astype(jnp.bfloat16)


def stage_layer(stage_ops):
    x_stage, stage_blocks, k_stage, v_stage, wq_stage, wkv_stage, wo_stage, wg_stage, wu_stage, wd_stage = stage_ops
    normed = rms_normalize(x_stage)
    q_heads = jnp.dot(normed, wq_stage, preferred_element_type=jnp.float32).astype(jnp.bfloat16).reshape(SLICE_LEN, N_HEADS, HEAD_DIM)
    kv_new = jnp.dot(normed, wkv_stage, preferred_element_type=jnp.float32).astype(jnp.bfloat16)
    k_all = jnp.concatenate([k_stage, kv_new[:, :QKV_WIDTH].reshape(SLICE_LEN, N_HEADS, HEAD_DIM)], axis=0)
    v_all = jnp.concatenate([v_stage, kv_new[:, QKV_WIDTH:].reshape(SLICE_LEN, N_HEADS, HEAD_DIM)], axis=0)
    key_pos = jnp.arange(P_MAX + SLICE_LEN)[None, :]
    query_pos = jnp.arange(SLICE_LEN)[:, None]
    visible = jnp.where(key_pos < P_MAX, key_pos < stage_blocks * SLICE_LEN, key_pos - P_MAX <= query_pos)
    attn_scale = HEAD_DIM ** -0.5

    def head_attend(head_ops):
        q_one, k_one, v_one = head_ops
        scores = jnp.dot(q_one, k_one.T, preferred_element_type=jnp.float32) * attn_scale
        scores = jnp.where(visible, scores, -1e30)
        row_peak = jnp.max(scores, axis=-1, keepdims=True)
        log_sum = row_peak + jnp.log(jnp.sum(jnp.exp(scores - row_peak), axis=-1, keepdims=True))
        prob_bf16 = jnp.exp(scores - log_sum).astype(jnp.bfloat16)
        return jnp.dot(prob_bf16, v_one, preferred_element_type=jnp.float32), log_sum[:, 0]

    head_out, head_lse = lax.map(head_attend, (q_heads.transpose(1, 0, 2), k_all.transpose(1, 0, 2), v_all.transpose(1, 0, 2)))
    attn_out = head_out.transpose(1, 0, 2).reshape(SLICE_LEN, QKV_WIDTH).astype(jnp.bfloat16)
    resid_out = (x_stage.astype(jnp.float32) + jnp.dot(attn_out, wo_stage, preferred_element_type=jnp.float32)).astype(jnp.bfloat16)
    mlp_in = rms_normalize(resid_out)
    gate_act = jnp.dot(mlp_in, wg_stage, preferred_element_type=jnp.float32)
    up_act = jnp.dot(mlp_in, wu_stage, preferred_element_type=jnp.float32)
    hidden = (jax.nn.silu(gate_act) * up_act).astype(jnp.bfloat16)
    y_stage = (resid_out.astype(jnp.float32) + jnp.dot(hidden, wd_stage, preferred_element_type=jnp.float32)).astype(jnp.bfloat16)
    return y_stage, head_lse.T


def reference(x_slice, slice_idx, k_cache, v_cache, w_q, w_kv, w_o, w_gate, w_up, w_down):
    stage_ops = (
        x_slice.reshape(STAGES, SLICE_LEN, D_MODEL),
        slice_idx,
        k_cache.reshape(STAGES, P_MAX, N_HEADS, HEAD_DIM),
        v_cache.reshape(STAGES, P_MAX, N_HEADS, HEAD_DIM),
        w_q, w_kv, w_o, w_gate, w_up, w_down,
    )
    y_stages, lse_stages = lax.map(stage_layer, stage_ops)
    y_next = jnp.roll(y_stages, 1, axis=0).reshape(STAGES * SLICE_LEN, D_MODEL)
    return y_next, lse_stages.reshape(STAGES * SLICE_LEN, N_HEADS)
```

```python
import functools
import math

import jax
import jax.numpy as jnp
from jax import lax
from jax.experimental import pallas as pl
from jax.experimental.pallas import tpu as pltpu
from jax.sharding import PartitionSpec as P

BF16 = jnp.bfloat16
F32 = jnp.float32
MASK_FLOOR = -1e30
LOG2E = math.log2(math.e)
LN2 = math.log(2.0)
MIB = 1 << 20
QH = 256
CHUNK = 64
HBM = pl.BlockSpec(memory_space=pltpu.HBM)
VMEM = pl.BlockSpec(memory_space=pltpu.VMEM)
SMEM = pl.BlockSpec(memory_space=pltpu.SMEM)


def dot(a, b):
    return lax.dot_general(a, b, (((1,), (0,)), ((), ())), preferred_element_type=F32)


def dot_t(a, b):
    return lax.dot_general(a, b, (((1,), (1,)), ((), ())), preferred_element_type=F32)


def rms_normalize(values):
    stats = values.astype(F32)
    inv_rms = lax.rsqrt(jnp.mean(stats * stats, axis=-1, keepdims=True) + 1e-6)
    return (stats * inv_rms).astype(BF16)


def ds(start, size):
    return pl.ds(pl.multiple_of(start, size), size)


def gather_item(n, first_pair, pairs, block_len, item, k_hbm, v_hbm, kt, vt, sem, act):
    block = item // pairs
    pair = item - block * pairs
    rows = ds(block * block_len, block_len)
    for side, (src, dst) in enumerate(((k_hbm, kt), (v_hbm, vt))):
        copy = pltpu.make_async_copy(src.at[rows, first_pair + pair], dst.at[pair, rows], sem.at[side])
        copy.start() if act == 'start' else copy.wait()


def gather_range(lo, hi, n, pairs, block_len, first_pair, k_hbm, v_hbm, kt, vt, sem, act):
    lo = jnp.minimum(lo, n * pairs)
    hi = jnp.minimum(hi, n * pairs)

    @pl.loop(lo, hi)
    def _(item):
        gather_item(n, first_pair, pairs, block_len, item, k_hbm, v_hbm, kt, vt, sem, act)


def qkv_kernel(pairs, block_len, n_ref, x_ref, wq_hbm, wkv_hbm, k_hbm, v_hbm, q_ref, kv_ref, kt, vt, a_ref, wbuf, wsem, gsem):
    n = n_ref[0]
    tile = wbuf.shape[3]
    q_steps = wq_hbm.shape[1] // (2 * tile)
    kv_steps = wkv_hbm.shape[1] // (2 * tile)
    steps = q_steps + kv_steps

    def fetch(step, slot):
        for half in range(2):
            @pl.when(step < q_steps)
            def _():
                pltpu.make_async_copy(wq_hbm.at[:, ds((2 * step + half) * tile, tile)], wbuf.at[slot, half], wsem.at[slot, half]).start()

            @pl.when(step >= q_steps)
            def _():
                pltpu.make_async_copy(wkv_hbm.at[:, ds((2 * (step - q_steps) + half) * tile, tile)], wbuf.at[slot, half], wsem.at[slot, half]).start()

    fetch(0, 0)
    a_ref[...] = rms_normalize(x_ref[...])
    share = (n * pairs + steps - 2) // (steps - 1)
    for phase, out_ref, first, count in ((0, q_ref, 0, q_steps), (1, kv_ref, q_steps, kv_steps)):
        def body(i, carry):
            step = first + i
            slot = lax.rem(step, 2)

            @pl.when(step + 1 < steps)
            def _():
                fetch(step + 1, 1 - slot)

            gather_range(step * share, (step + 1) * share, n, pairs, block_len, 0, k_hbm, v_hbm, kt, vt, gsem, 'start')
            for half in range(2):
                pltpu.make_async_copy(wq_hbm.at[:, 0:tile], wbuf.at[slot, half], wsem.at[slot, half]).wait()
                out_ref[:, ds((2 * i + half) * tile, tile)] = dot(a_ref[...], wbuf[slot, half]).astype(BF16)
            return carry

        lax.fori_loop(0, count, body, 0)
    gather_range(0, n * pairs, n, pairs, block_len, 0, k_hbm, v_hbm, kt, vt, gsem, 'wait')


def parity_max(x):
    x = jnp.maximum(x, pltpu.roll(x, 2, 0))
    return jnp.maximum(x, pltpu.roll(x, 4, 0))


def parity_sum(x):
    x = x + pltpu.roll(x, 2, 0)
    return x + pltpu.roll(x, 4, 0)


def attn_kernel(first_pair, gather_pairs, block_len, n_ref, q_ref, kn_ref, vn_ref, kt_ref, vt_ref, *rest):
    if gather_pairs:
        k_hbm, v_hbm, o_ref, lse_ref, kt_next, vt_next, *rest = rest
    else:
        o_ref, lse_ref, *rest = rest
    m_ref, l_ref, acc_ref, s_ref, p_ref, mx_ref, al_ref, gsem = rest
    n = n_ref[0]
    pairs = kt_ref.shape[0]
    scale = LOG2E * 128 ** -0.5
    keys = 2 * block_len
    if gather_pairs:
        gather_range(0, n * gather_pairs, n, gather_pairs, block_len, first_pair + pairs, k_hbm, v_hbm, kt_next, vt_next, gsem, 'start')

    def cols_of(p):
        return ds((first_pair + p) * 256, 256)

    def new_keys(p, carry):
        kn = kn_ref[:, cols_of(p)]
        vn = vn_ref[:, cols_of(p)]
        state = [[None, None], [None, None]]
        for h in range(2):
            hs = slice(h * 128, h * 128 + 128)
            kh = kn[:, hs]
            vth = vn[:, hs].T
            for qh in range(2):
                rows = QH * (qh + 1)
                qb = q_ref[qh * QH:(qh + 1) * QH, cols_of(p)]
                s = dot_t(kh[:rows], qb[:, hs])
                key = lax.broadcasted_iota(jnp.int32, (QH, QH), 0)
                query = lax.broadcasted_iota(jnp.int32, (QH, QH), 1)
                tri = jnp.where(key <= query, s[rows - QH:], MASK_FLOOR)
                s = tri if qh == 0 else jnp.concatenate([s[:QH], tri], axis=0)
                m = jnp.max(s, axis=0, keepdims=True) * scale
                e = jnp.exp2(s * scale - m)
                state[qh][h] = (m, jnp.sum(e, axis=0, keepdims=True))
                acc_ref[p, qh, hs] = dot(vth[:, :rows], e.astype(BF16))
        even8 = lax.broadcasted_iota(jnp.int32, (8, QH), 0) % 2 == 0
        for qh in range(2):
            (m0, l0), (m1, l1) = state[qh]
            m_ref[p, qh] = jnp.where(even8, jnp.broadcast_to(m0, (8, QH)), jnp.broadcast_to(m1, (8, QH)))
            l_ref[p, qh] = jnp.where(even8, jnp.broadcast_to(l0, (8, QH)), jnp.broadcast_to(l1, (8, QH))) * 0.25
        return carry

    lax.fori_loop(0, pairs, new_keys, 0)

    def k_block(p, b):
        kx = kt_ref[p, ds(b * keys, keys), :]
        even = lax.broadcasted_iota(jnp.int32, kx.shape, 0) % 2 == 0
        zero = jnp.zeros_like(kx)
        return jnp.concatenate([jnp.where(even, kx, zero), jnp.where(even, zero, kx)], axis=1)

    def v_block(p, b):
        vx = vt_ref[p, ds(b * keys, keys), :].T
        even = lax.broadcasted_iota(jnp.int32, vx.shape, 1) % 2 == 0
        zero = jnp.zeros_like(vx)
        return jnp.concatenate([jnp.where(even, vx, zero), jnp.where(even, zero, vx)], axis=0)

    def scores(ke, p, qh):
        s = dot_t(ke, q_ref[qh * QH:(qh + 1) * QH, cols_of(p)])
        s_ref[qh] = s
        mx_ref[qh] = jnp.max(s.reshape(keys // 8, 8, QH), axis=0)

    def weights(p, qh):
        m_old = m_ref[p, qh]
        m = jnp.maximum(m_old, parity_max(mx_ref[qh]) * scale)
        alpha = jnp.exp2(m_old - m)
        total = l_ref[p, qh] * alpha
        for r in range(0, keys, CHUNK):
            s3 = s_ref[qh, r:r + CHUNK].reshape(CHUNK // 8, 8, QH)
            e = jnp.exp2(s3 * scale - m[None])
            total = total + jnp.sum(e, axis=0)
            p_ref[qh, r:r + CHUNK] = e.reshape(CHUNK, QH).astype(BF16)
        l_ref[p, qh] = total
        m_ref[p, qh] = m
        al_ref[qh] = alpha

    def values(ve, p, qh):
        out = dot(ve, p_ref[qh])
        alpha = al_ref[qh]
        acc_ref[p, qh, 0:128] = acc_ref[p, qh, 0:128] * alpha[0:1] + out[0:128]
        acc_ref[p, qh, 128:256] = acc_ref[p, qh, 128:256] * alpha[1:2] + out[128:256]

    @pl.when(n > 0)
    def _():
        ke = k_block(0, 0)
        scores(ke, 0, 0)
        weights(0, 0)
        scores(ke, 0, 1)

        def body(t, carry):
            pp, bp = carry
            wrap = bp + 1 == n
            p = jnp.where(wrap, pp + 1, pp)
            b = jnp.where(wrap, 0, bp + 1)
            ve = v_block(pp, bp)
            ke = k_block(p, b)
            scores(ke, p, 0)
            values(ve, pp, 0)
            weights(pp, 1)
            values(ve, pp, 1)
            scores(ke, p, 1)
            weights(p, 0)
            return p, b

        pp, bp = lax.fori_loop(1, pairs * n, body, (jnp.int32(0), jnp.int32(0)))
        ve = v_block(pp, bp)
        values(ve, pp, 0)
        weights(pp, 1)
        values(ve, pp, 1)

    def finish(p, carry):
        for qh in range(2):
            l = parity_sum(l_ref[p, qh])
            lse_ref[p, :, qh * QH:(qh + 1) * QH] = ((m_ref[p, qh] + jnp.log2(l)) * LN2)[0:2]
            inv = 1.0 / l
            o = jnp.concatenate([acc_ref[p, qh, h * 128:(h + 1) * 128] * inv[h:h + 1] for h in range(2)], axis=0)
            o_ref[qh * QH:(qh + 1) * QH, ds(p * 256, 256)] = o.T.astype(BF16)
        return carry

    lax.fori_loop(0, pairs, finish, 0)
    if gather_pairs:
        gather_range(0, n * gather_pairs, n, gather_pairs, block_len, first_pair + pairs, k_hbm, v_hbm, kt_next, vt_next, gsem, 'wait')


def out_kernel(x_ref, oa_ref, ob_ref, wo_hbm, h_ref, b_ref, wbuf, wsem):
    tile = wbuf.shape[2]
    steps = wo_hbm.shape[1] // tile
    half = oa_ref.shape[1]

    def fetch(i):
        return pltpu.make_async_copy(wo_hbm.at[:, ds(i * tile, tile)], wbuf.at[i], wsem.at[i])

    for i in range(steps):
        fetch(i).start()

    def body(i, sq):
        fetch(i).wait()
        part = dot(oa_ref[...], wbuf[i, :half]) + dot(ob_ref[...], wbuf[i, half:])
        cols = ds(i * tile, tile)
        h = (x_ref[:, cols].astype(F32) + part).astype(BF16)
        h_ref[:, cols] = h
        h = h.astype(F32)
        return sq + jnp.sum(h * h, axis=1, keepdims=True)

    sq = lax.fori_loop(0, steps, body, jnp.zeros((x_ref.shape[0], 1), F32))
    inv_rms = lax.rsqrt(sq * (1.0 / h_ref.shape[1]) + 1e-6)
    b_ref[...] = (h_ref[...].astype(F32) * inv_rms).astype(BF16)


def gate_up_kernel(b_ref, wg_hbm, wu_hbm, hid_ref, wbuf, g_ref, u_ref, wsem):
    tile = wbuf.shape[3]
    steps = wg_hbm.shape[1] // tile

    def fetch(i, slot):
        return [pltpu.make_async_copy(w.at[:, ds(i * tile, tile)], wbuf.at[slot, j], wsem.at[slot, j]) for j, w in enumerate((wg_hbm, wu_hbm))]

    def act(g, u):
        return (g * jax.nn.sigmoid(g) * u).astype(BF16)

    for c in fetch(0, 0):
        c.start()

    def step(i, first):
        slot = lax.rem(i, 2)

        @pl.when(i + 1 < steps)
        def _():
            for c in fetch(i + 1, 1 - slot):
                c.start()

        for c in fetch(i, slot):
            c.wait()
        if not first:
            hid_ref[:, ds((2 * i - 1) * 256, 256)] = act(g_ref[...], u_ref[...])
        b = b_ref[...]
        g = dot(b, wbuf[slot, 0, :, 0:256])
        u = dot(b, wbuf[slot, 1, :, 0:256])
        hid_ref[:, ds(2 * i * 256, 256)] = act(g, u)
        g_ref[...] = dot(b, wbuf[slot, 0, :, 256:512])
        u_ref[...] = dot(b, wbuf[slot, 1, :, 256:512])

    step(0, True)

    @pl.loop(1, steps)
    def _(i):
        step(i, False)

    hid_ref[:, (2 * steps - 1) * 256:2 * steps * 256] = act(g_ref[...], u_ref[...])


def down_kernel(stages, hid_ref, h_ref, wd_hbm, y_ref, wbuf, ybuf, wsem, send_sem, recv_sem):
    me = lax.axis_index('pipe')
    right = lax.rem(me + 1, stages)
    left = lax.rem(me + stages - 1, stages)
    barrier = pltpu.get_barrier_semaphore()
    pl.semaphore_signal(barrier, inc=1, device_id={'pipe': left}, device_id_type=pl.DeviceIdType.MESH)
    tile = wbuf.shape[2]
    steps = wd_hbm.shape[1] // tile
    rows = h_ref.shape[0] // 2

    def fetch(i, slot):
        return pltpu.make_async_copy(wd_hbm.at[:, ds(i * tile, tile)], wbuf.at[slot], wsem.at[slot])

    def send(i, mh):
        cols = ds(i * tile, tile)
        part = pl.ds(mh * rows, rows)
        return pltpu.make_async_remote_copy(
            src_ref=ybuf.at[part, cols], dst_ref=y_ref.at[part, cols], send_sem=send_sem.at[i, mh],
            recv_sem=recv_sem.at[i, mh], device_id={'pipe': right}, device_id_type=pl.DeviceIdType.MESH)

    fetch(0, 0).start()
    for i in range(steps):
        slot = i % 2
        if i + 1 < steps:
            fetch(i + 1, 1 - slot).start()
        fetch(i, slot).wait()
        for mh in range(2):
            part = slice(mh * rows, (mh + 1) * rows)
            cols = slice(i * tile, (i + 1) * tile)
            out = dot(hid_ref[part, :], wbuf[slot])
            ybuf[part, cols] = (h_ref[part, cols].astype(F32) + out).astype(BF16)
            if i == 0 and mh == 0:
                pl.semaphore_wait(barrier, 1)
            send(i, mh).start()
    for i in range(steps):
        for mh in range(2):
            send(i, mh).wait()


def params(limit_mib, **kwargs):
    return pltpu.CompilerParams(vmem_limit_bytes=limit_mib * MIB, **kwargs)


def solution(mesh):
    stages = mesh.shape['pipe']

    def device_step(x, slice_idx, k_cache, v_cache, w_q, w_kv, w_o, w_gate, w_up, w_down):
        seq, width = x.shape
        cache_len, n_heads, head_dim = k_cache.shape
        pairs = n_heads // 2
        half = pairs // 2
        w_q, w_kv, w_o, w_gate, w_up, w_down = (w[0] for w in (w_q, w_kv, w_o, w_gate, w_up, w_down))
        ff = w_gate.shape[1]
        k4 = k_cache.reshape(cache_len, pairs, 2, head_dim)
        v4 = v_cache.reshape(cache_len, pairs, 2, head_dim)
        gathered = pltpu.VMEM((half, cache_len, 2, head_dim), BF16)
        dma = pltpu.SemaphoreType.DMA

        q, kv, kt_a, vt_a = pl.pallas_call(
            functools.partial(qkv_kernel, half, seq), name='qkv',
            in_specs=[SMEM, VMEM, HBM, HBM, HBM, HBM], out_specs=[VMEM] * 4,
            out_shape=[pltpu.VMEM((seq, width), BF16), pltpu.VMEM((seq, 2 * width), BF16), gathered, gathered],
            scratch_shapes=[pltpu.VMEM((seq, width), BF16), pltpu.VMEM((2, 2, width, 512), BF16), dma((2, 2)), dma((2,))],
            compiler_params=params(20),
        )(slice_idx, x, w_q, w_kv, k4, v4)

        def attention(first_pair, kt, vt, more):
            native = (half, 2 * cache_len, head_dim)
            outs = [pltpu.VMEM((seq, width // 2), BF16), jax.ShapeDtypeStruct((half, 2, seq), F32)]
            return pl.pallas_call(
                functools.partial(attn_kernel, first_pair, half if more else 0, seq), name='attn',
                in_specs=[SMEM] + [VMEM] * 5 + [HBM, HBM] * more, out_specs=[VMEM] * (2 + 2 * more),
                out_shape=outs + [gathered, gathered] * more,
                scratch_shapes=[pltpu.VMEM((half, 2, 8, QH), F32), pltpu.VMEM((half, 2, 8, QH), F32), pltpu.VMEM((half, 2, 256, QH), F32),
                                pltpu.VMEM((2, 2 * seq, QH), F32), pltpu.VMEM((2, 2 * seq, QH), BF16),
                                pltpu.VMEM((2, 8, QH), F32), pltpu.VMEM((2, 8, QH), F32), dma((2,))],
                compiler_params=params(12),
            )(slice_idx, q, kv[:, :width], kv[:, width:], kt.reshape(native), vt.reshape(native), *((k4, v4) if more else ()))

        o_a, lse_a, kt_b, vt_b = attention(0, kt_a, vt_a, 1)
        o_b, lse_b = attention(half, kt_b, vt_b, 0)
        lse = jnp.concatenate([lse_a, lse_b]).reshape(n_heads, seq).T

        h, b = pl.pallas_call(
            out_kernel, name='proj_out', in_specs=[VMEM, VMEM, VMEM, HBM], out_specs=[VMEM, VMEM],
            out_shape=[pltpu.VMEM((seq, width), BF16)] * 2,
            scratch_shapes=[pltpu.VMEM((4, width, width // 4), BF16), dma((4,))],
            compiler_params=params(16),
        )(x, o_a, o_b, w_o)

        hidden = pl.pallas_call(
            gate_up_kernel, name='gate_up', in_specs=[VMEM, HBM, HBM], out_specs=VMEM,
            out_shape=pltpu.VMEM((seq, ff), BF16),
            scratch_shapes=[pltpu.VMEM((2, 2, width, 512), BF16), pltpu.VMEM((seq, 256), F32), pltpu.VMEM((seq, 256), F32), dma((2, 2))],
            compiler_params=params(16),
        )(b, w_gate, w_up)

        y_next = pl.pallas_call(
            functools.partial(down_kernel, stages), name='down', in_specs=[VMEM, VMEM, HBM], out_specs=HBM,
            out_shape=jax.ShapeDtypeStruct((seq, width), BF16),
            scratch_shapes=[pltpu.VMEM((2, ff, 512), BF16), pltpu.VMEM((seq, width), BF16), dma((2,)), dma((4, 2)), dma((4, 2))],
            compiler_params=params(30, collective_id=0, has_side_effects=True),
        )(hidden, h, w_down)
        return y_next, lse

    rows_spec = P(('data', 'pipe'), None)
    cache_spec = P(('data', 'pipe'), None, None)
    stage_spec = P('pipe', None, None)
    return jax.shard_map(
        device_step,
        mesh=mesh,
        in_specs=(rows_spec, P(('data', 'pipe')), cache_spec, cache_spec) + (stage_spec,) * 6,
        out_specs=(rows_spec, rows_spec),
        check_vma=False,
    )
```

```python
import functools
import math

import jax
import jax.numpy as jnp
from jax import lax
from jax.experimental import pallas as pl
from jax.experimental.pallas import tpu as pltpu
from jax.sharding import PartitionSpec as P

BF16 = jnp.bfloat16
F32 = jnp.float32
MASK_FLOOR = -1e30
LOG2E = math.log2(math.e)
LN2 = math.log(2.0)
MIB = 1 << 20
QH = 256
CHUNK = 64
HBM = pl.BlockSpec(memory_space=pltpu.HBM)
VMEM = pl.BlockSpec(memory_space=pltpu.VMEM)
SMEM = pl.BlockSpec(memory_space=pltpu.SMEM)


def in_hbm(x):
    return pltpu.with_memory_space_constraint(x, pltpu.HBM)


def dot(a, b):
    return lax.dot_general(a, b, (((1,), (0,)), ((), ())), preferred_element_type=F32)


def dot_t(a, b):
    return lax.dot_general(a, b, (((1,), (1,)), ((), ())), preferred_element_type=F32)


def rms_normalize(values):
    stats = values.astype(F32)
    inv_rms = lax.rsqrt(jnp.mean(stats * stats, axis=-1, keepdims=True) + 1e-6)
    return (stats * inv_rms).astype(BF16)


def ds(start, size):
    return pl.ds(pl.multiple_of(start, size), size)


def gather_item(n, first_pair, pairs, block_len, item, k_hbm, v_hbm, kt, vt, sem, act):
    block = item // pairs
    pair = item - block * pairs
    rows = ds(block * block_len, block_len)
    for side, (src, dst) in enumerate(((k_hbm, kt), (v_hbm, vt))):
        copy = pltpu.make_async_copy(src.at[rows, first_pair + pair], dst.at[pair, rows], sem.at[side])
        copy.start() if act == 'start' else copy.wait()


def gather_range(lo, hi, n, pairs, block_len, first_pair, k_hbm, v_hbm, kt, vt, sem, act):
    lo = jnp.minimum(lo, n * pairs)
    hi = jnp.minimum(hi, n * pairs)

    @pl.loop(lo, hi)
    def _(item):
        gather_item(n, first_pair, pairs, block_len, item, k_hbm, v_hbm, kt, vt, sem, act)


def qkv_kernel(pairs, block_len, n_ref, x_hbm, wq_hbm, wkv_hbm, k_hbm, v_hbm, q_ref, kv_ref, kt, vt, x_ref, a_ref, wbuf, xsem, wsem, gsem):
    n = n_ref[0]
    x_copy = pltpu.make_async_copy(x_hbm, x_ref, xsem)
    x_copy.start()
    tile = wbuf.shape[3]
    q_steps = wq_hbm.shape[1] // (2 * tile)
    kv_steps = wkv_hbm.shape[1] // (2 * tile)
    steps = q_steps + kv_steps

    def fetch(step, slot):
        for half in range(2):
            @pl.when(step < q_steps)
            def _():
                pltpu.make_async_copy(wq_hbm.at[:, ds((2 * step + half) * tile, tile)], wbuf.at[slot, half], wsem.at[slot, half]).start()

            @pl.when(step >= q_steps)
            def _():
                pltpu.make_async_copy(wkv_hbm.at[:, ds((2 * (step - q_steps) + half) * tile, tile)], wbuf.at[slot, half], wsem.at[slot, half]).start()

    fetch(0, 0)
    x_copy.wait()
    a_ref[...] = rms_normalize(x_ref[...])
    share = (n * pairs + steps - 2) // (steps - 1)
    for phase, out_ref, first, count in ((0, q_ref, 0, q_steps), (1, kv_ref, q_steps, kv_steps)):
        def body(i, carry):
            step = first + i
            slot = lax.rem(step, 2)

            @pl.when(step + 1 < steps)
            def _():
                fetch(step + 1, 1 - slot)

            gather_range(step * share, (step + 1) * share, n, pairs, block_len, 0, k_hbm, v_hbm, kt, vt, gsem, 'start')
            for half in range(2):
                pltpu.make_async_copy(wq_hbm.at[:, 0:tile], wbuf.at[slot, half], wsem.at[slot, half]).wait()
                out_ref[:, ds((2 * i + half) * tile, tile)] = dot(a_ref[...], wbuf[slot, half]).astype(BF16)
            return carry

        lax.fori_loop(0, count, body, 0)
    gather_range(0, n * pairs, n, pairs, block_len, 0, k_hbm, v_hbm, kt, vt, gsem, 'wait')


def parity_max(x):
    x = jnp.maximum(x, pltpu.roll(x, 2, 0))
    return jnp.maximum(x, pltpu.roll(x, 4, 0))


def parity_sum(x):
    x = x + pltpu.roll(x, 2, 0)
    return x + pltpu.roll(x, 4, 0)


def project_out(x_ref, o_refs, fetch_wo, wo_ref, h_ref, b_ref):
    width = h_ref.shape[1]
    steps = width // wo_ref.shape[2]

    def project(i, sq):
        cols = ds(i * 512, 512)
        slot = lax.rem(i, 2)
        fetch_wo(i, slot).wait()
        part = dot(jnp.concatenate([o[...] for o in o_refs], axis=1), wo_ref[slot])

        @pl.when(i + 2 < steps)
        def _():
            fetch_wo(i + 2, slot).start()

        h = (x_ref[:, cols].astype(F32) + part).astype(BF16)
        h_ref[:, cols] = h
        h = h.astype(F32)
        return sq + jnp.sum(h * h, axis=1, keepdims=True)

    sq = lax.fori_loop(0, steps, project, jnp.zeros((x_ref.shape[0], 1), F32))
    inv_rms = lax.rsqrt(sq * (1.0 / width) + 1e-6)
    b_ref[...] = (h_ref[...].astype(F32) * inv_rms).astype(BF16)


def attn_kernel(first_pair, gather_pairs, n_others, block_len, n_ref, q_ref, kv_ref, kt_ref, vt_ref, *rest):
    if gather_pairs:
        k_hbm, v_hbm, lse_ref, o_ref, kt_next, vt_next, *rest = rest
    else:
        others, rest = rest[:n_others], rest[n_others:]
        x_hbm, wo_hbm, lse_ref, h_ref, b_ref, x_ref, wo_ref, o_ref, wo_sem, *rest = rest
    m_ref, l_ref, acc_ref, s_ref, p_ref, mx_ref, al_ref, gsem = rest
    n = n_ref[0]
    pairs = kt_ref.shape[0]
    scale = LOG2E * 128 ** -0.5
    keys = 2 * block_len
    if gather_pairs:
        gather_range(0, n * gather_pairs, n, gather_pairs, block_len, first_pair + pairs, k_hbm, v_hbm, kt_next, vt_next, gsem, 'start')
    else:
        def fetch_wo(i, slot):
            return pltpu.make_async_copy(wo_hbm.at[:, ds(i * 512, 512)], wo_ref.at[slot], wo_sem.at[slot])

        x_copy = pltpu.make_async_copy(x_hbm, x_ref, gsem.at[0])
        x_copy.start()
        fetch_wo(0, 0).start()
        fetch_wo(1, 1).start()

    def cols_of(p):
        return ds((first_pair + p) * 256, 256)

    def new_keys(p, carry):
        kn = kv_ref[:, cols_of(p)]
        vn = kv_ref[:, ds((first_pair + p) * 256 + q_ref.shape[1], 256)]
        state = [[None, None], [None, None]]
        for h in range(2):
            hs = slice(h * 128, h * 128 + 128)
            kh = kn[:, hs]
            vth = vn[:, hs].T
            for qh in range(2):
                rows = QH * (qh + 1)
                qb = q_ref[qh * QH:(qh + 1) * QH, cols_of(p)]
                s = dot_t(kh[:rows], qb[:, hs])
                key = lax.broadcasted_iota(jnp.int32, (QH, QH), 0)
                query = lax.broadcasted_iota(jnp.int32, (QH, QH), 1)
                tri = jnp.where(key <= query, s[rows - QH:], MASK_FLOOR)
                s = tri if qh == 0 else jnp.concatenate([s[:QH], tri], axis=0)
                m = jnp.max(s, axis=0, keepdims=True) * scale
                e = jnp.exp2(s * scale - m)
                state[qh][h] = (m, jnp.sum(e, axis=0, keepdims=True))
                acc_ref[p, qh, hs] = dot(vth[:, :rows], e.astype(BF16))
        even8 = lax.broadcasted_iota(jnp.int32, (8, QH), 0) % 2 == 0
        for qh in range(2):
            (m0, l0), (m1, l1) = state[qh]
            m_ref[p, qh] = jnp.where(even8, jnp.broadcast_to(m0, (8, QH)), jnp.broadcast_to(m1, (8, QH)))
            l_ref[p, qh] = jnp.where(even8, jnp.broadcast_to(l0, (8, QH)), jnp.broadcast_to(l1, (8, QH))) * 0.25
        return carry

    lax.fori_loop(0, pairs, new_keys, 0)

    def k_block(p, b):
        kx = kt_ref[p, ds(b * keys, keys), :]
        even = lax.broadcasted_iota(jnp.int32, kx.shape, 0) % 2 == 0
        zero = jnp.zeros_like(kx)
        return jnp.concatenate([jnp.where(even, kx, zero), jnp.where(even, zero, kx)], axis=1)

    def v_block(p, b):
        vx = vt_ref[p, ds(b * keys, keys), :].T
        even = lax.broadcasted_iota(jnp.int32, vx.shape, 1) % 2 == 0
        zero = jnp.zeros_like(vx)
        return jnp.concatenate([jnp.where(even, vx, zero), jnp.where(even, zero, vx)], axis=0)

    def scores(ke, p, qh):
        s = dot_t(ke, q_ref[qh * QH:(qh + 1) * QH, cols_of(p)])
        s_ref[qh] = s
        mx_ref[qh] = jnp.max(s.reshape(keys // 8, 8, QH), axis=0)

    def weights(p, qh):
        m_old = m_ref[p, qh]
        m = jnp.maximum(m_old, parity_max(mx_ref[qh]) * scale)
        alpha = jnp.exp2(m_old - m)
        total = l_ref[p, qh] * alpha
        for r in range(0, keys, CHUNK):
            s3 = s_ref[qh, r:r + CHUNK].reshape(CHUNK // 8, 8, QH)
            e = jnp.exp2(s3 * scale - m[None])
            total = total + jnp.sum(e, axis=0)
            p_ref[qh, r:r + CHUNK] = e.reshape(CHUNK, QH).astype(BF16)
        l_ref[p, qh] = total
        m_ref[p, qh] = m
        al_ref[qh] = alpha

    def values(ve, p, qh):
        out = dot(ve, p_ref[qh])
        alpha = al_ref[qh]
        acc_ref[p, qh, 0:128] = acc_ref[p, qh, 0:128] * alpha[0:1] + out[0:128]
        acc_ref[p, qh, 128:256] = acc_ref[p, qh, 128:256] * alpha[1:2] + out[128:256]

    @pl.when(n > 0)
    def _():
        ke = k_block(0, 0)
        scores(ke, 0, 0)
        weights(0, 0)
        scores(ke, 0, 1)

        def body(t, carry):
            pp, bp = carry
            wrap = bp + 1 == n
            p = jnp.where(wrap, pp + 1, pp)
            b = jnp.where(wrap, 0, bp + 1)
            ve = v_block(pp, bp)
            ke = k_block(p, b)
            scores(ke, p, 0)
            values(ve, pp, 0)
            weights(pp, 1)
            values(ve, pp, 1)
            scores(ke, p, 1)
            weights(p, 0)
            return p, b

        pp, bp = lax.fori_loop(1, pairs * n, body, (jnp.int32(0), jnp.int32(0)))
        ve = v_block(pp, bp)
        values(ve, pp, 0)
        weights(pp, 1)
        values(ve, pp, 1)

    def finish(p, carry):
        for qh in range(2):
            l = parity_sum(l_ref[p, qh])
            lse_ref[p, :, qh * QH:(qh + 1) * QH] = ((m_ref[p, qh] + jnp.log2(l)) * LN2)[0:2]
            inv = 1.0 / l
            o = jnp.concatenate([acc_ref[p, qh, h * 128:(h + 1) * 128] * inv[h:h + 1] for h in range(2)], axis=0)
            o_ref[qh * QH:(qh + 1) * QH, ds(p * 256, 256)] = o.T.astype(BF16)
        return carry

    lax.fori_loop(0, pairs, finish, 0)
    if gather_pairs:
        gather_range(0, n * gather_pairs, n, gather_pairs, block_len, first_pair + pairs, k_hbm, v_hbm, kt_next, vt_next, gsem, 'wait')
    else:
        x_copy.wait()
        project_out(x_ref, (*others, o_ref), fetch_wo, wo_ref, h_ref, b_ref)


def mlp_kernel(stages, h_ref, b_ref, wg_hbm, wu_hbm, wd_hbm, y_ref,
               hid_ref, gu_buf, g_ref, u_ref, wd_buf, ybuf, gu_sem, wd_sem, send_sem, recv_sem):
    me = lax.axis_index('pipe')
    right = lax.rem(me + 1, stages)
    left = lax.rem(me + stages - 1, stages)
    barrier = pltpu.get_barrier_semaphore()
    pl.semaphore_signal(barrier, inc=1, device_id={'pipe': left}, device_id_type=pl.DeviceIdType.MESH)
    width = h_ref.shape[1]
    gu_tile = gu_buf.shape[3]
    gu_steps = wg_hbm.shape[1] // gu_tile
    wd_tile = wd_buf.shape[2]
    wd_steps = width // wd_tile

    def fetch_gu(i, slot):
        return [pltpu.make_async_copy(w.at[:, ds(i * gu_tile, gu_tile)], gu_buf.at[slot, j], gu_sem.at[slot, j]) for j, w in enumerate((wg_hbm, wu_hbm))]

    def fetch_wd(i):
        slot = lax.rem(i, 2)
        return pltpu.make_async_copy(wd_hbm.at[:, ds(i * wd_tile, wd_tile)], wd_buf.at[slot], wd_sem.at[slot])

    for i in range(2):
        for c in fetch_gu(i, i):
            c.start()

    def act(g, u):
        return (g * jax.nn.sigmoid(g) * u).astype(BF16)

    def step(i, first):
        slot = lax.rem(i, 2)
        for c in fetch_gu(i, slot):
            c.wait()
        if not first:
            hid_ref[:, ds((2 * i - 1) * 256, 256)] = act(g_ref[...], u_ref[...])
        b = b_ref[...]
        g = dot(b, gu_buf[slot, 0, :, 0:256])
        u = dot(b, gu_buf[slot, 1, :, 0:256])
        hid_ref[:, ds(2 * i * 256, 256)] = act(g, u)
        g_ref[...] = dot(b, gu_buf[slot, 0, :, 256:512])
        u_ref[...] = dot(b, gu_buf[slot, 1, :, 256:512])

        @pl.when(i + 2 < gu_steps)
        def _():
            for c in fetch_gu(i + 2, slot):
                c.start()

    step(0, True)
    for i in range(2):
        fetch_wd(i).start()

    @pl.loop(1, gu_steps)
    def _(i):
        step(i, False)

    hid_ref[:, (2 * gu_steps - 1) * 256:2 * gu_steps * 256] = act(g_ref[...], u_ref[...])

    rows = h_ref.shape[0] // 2

    def send(i, mh):
        cols = ds(i * wd_tile, wd_tile)
        part = pl.ds(mh * rows, rows)
        return pltpu.make_async_remote_copy(
            src_ref=ybuf.at[part, cols], dst_ref=y_ref.at[part, cols], send_sem=send_sem.at[i, mh],
            recv_sem=recv_sem.at[i, mh], device_id={'pipe': right}, device_id_type=pl.DeviceIdType.MESH)

    pl.semaphore_wait(barrier, 1)

    @pl.loop(0, wd_steps)
    def _(i):
        slot = lax.rem(i, 2)
        fetch_wd(i).wait()
        cols = ds(i * wd_tile, wd_tile)
        for mh in range(2):
            part = slice(mh * rows, (mh + 1) * rows)
            out = dot(hid_ref[part, :], wd_buf[slot])
            ybuf[part, cols] = (h_ref[part, cols].astype(F32) + out).astype(BF16)
            send(i, mh).start()

        @pl.when(i + 2 < wd_steps)
        def _():
            fetch_wd(i + 2).start()

    @pl.loop(0, wd_steps)
    def _(i):
        for mh in range(2):
            send(i, mh).wait()


def params(limit_mib, **kwargs):
    return pltpu.CompilerParams(vmem_limit_bytes=limit_mib * MIB, **kwargs)


def solution(mesh):
    stages = mesh.shape['pipe']

    def device_step(x, slice_idx, k_cache, v_cache, w_q, w_kv, w_o, w_gate, w_up, w_down):
        seq, width = x.shape
        cache_len, n_heads, head_dim = k_cache.shape
        pairs = n_heads // 2
        x, w_q, w_kv, w_o, w_gate, w_up, w_down = map(in_hbm, (x, w_q[0], w_kv[0], w_o[0], w_gate[0], w_up[0], w_down[0]))
        ff = w_gate.shape[1]
        k4 = in_hbm(k_cache.reshape(cache_len, pairs, 2, head_dim))
        v4 = in_hbm(v_cache.reshape(cache_len, pairs, 2, head_dim))
        phases = (2, 3, 3)
        gathered = lambda count: [pltpu.VMEM((count, cache_len, 2, head_dim), BF16)] * 2
        big = lambda *shape: pltpu.VMEM(shape, BF16)
        dma = pltpu.SemaphoreType.DMA

        q, kv, kt, vt = pl.pallas_call(
            functools.partial(qkv_kernel, phases[0], seq), name='qkv',
            in_specs=[SMEM, HBM, HBM, HBM, HBM, HBM], out_specs=[VMEM] * 4,
            out_shape=[pltpu.VMEM((seq, width), BF16), pltpu.VMEM((seq, 2 * width), BF16)] + gathered(phases[0]),
            scratch_shapes=[pltpu.VMEM((seq, width), BF16), pltpu.VMEM((seq, width), BF16), pltpu.VMEM((2, 2, width, 512), BF16), dma, dma((2, 2)), dma((2,))],
            compiler_params=params(17),
        )(slice_idx, x, w_q, w_kv, k4, v4)

        outs, lses, first = [], [], 0
        for phase, count in enumerate(phases):
            last = phase == len(phases) - 1
            native = (count, 2 * cache_len, head_dim)
            lse_shape = jax.ShapeDtypeStruct((count, 2, seq), F32)
            mine = big(seq, count * 256)
            if last:
                extra = [big(seq, width), big(2, width, 512), mine, dma((2,))]
                shapes = [lse_shape, big(seq, width), big(seq, width)]
                more = (*outs, x, w_o)
            else:
                extra = []
                shapes = [lse_shape, mine] + gathered(phases[phase + 1])
                more = (k4, v4)
            lse, *res = pl.pallas_call(
                functools.partial(attn_kernel, first, 0 if last else phases[phase + 1], len(outs) if last else 0, seq), name='attn',
                in_specs=[SMEM] + [VMEM] * (4 + (len(outs) if last else 0)) + [HBM, HBM], out_specs=[VMEM] * len(shapes), out_shape=shapes,
                scratch_shapes=extra + [pltpu.VMEM((count, 2, 8, QH), F32), pltpu.VMEM((count, 2, 8, QH), F32), pltpu.VMEM((count, 2, 256, QH), F32),
                                        pltpu.VMEM((2, 2 * seq, QH), F32), big(2, 2 * seq, QH),
                                        pltpu.VMEM((2, 8, QH), F32), pltpu.VMEM((2, 8, QH), F32), dma((2,))],
                compiler_params=params(17 if last else 9),
            )(slice_idx, q, kv, kt.reshape(native), vt.reshape(native), *more)
            lses.append(lse)
            first += count
            if last:
                h, b = res
            else:
                o, kt, vt = res
                outs.append(o)
        lse = jnp.concatenate(lses).reshape(n_heads, seq).T

        y_next = pl.pallas_call(
            functools.partial(mlp_kernel, stages), name='mlp', in_specs=[VMEM] * 2 + [HBM] * 3, out_specs=HBM,
            out_shape=jax.ShapeDtypeStruct((seq, width), BF16),
            scratch_shapes=[big(seq, ff), big(2, 2, width, 512), pltpu.VMEM((seq, 256), F32), pltpu.VMEM((seq, 256), F32),
                            big(2, ff, 256), big(seq, width), dma((2, 2)), dma((2,)), dma((8, 2)), dma((8, 2))],
            compiler_params=params(32, collective_id=0, has_side_effects=True),
        )(h, b, w_gate, w_up, w_down)
        return y_next, lse

    rows_spec = P(('data', 'pipe'), None)
    cache_spec = P(('data', 'pipe'), None, None)
    stage_spec = P('pipe', None, None)
    return jax.shard_map(
        device_step,
        mesh=mesh,
        in_specs=(rows_spec, P(('data', 'pipe')), cache_spec, cache_spec) + (stage_spec,) * 6,
        out_specs=(rows_spec, rows_spec),
        check_vma=False,
    )
```

```python
import functools
import math

import jax
import jax.numpy as jnp
from jax import lax
from jax.experimental import pallas as pl
from jax.experimental.pallas import tpu as pltpu
from jax.sharding import PartitionSpec as P

BF16 = jnp.bfloat16
F32 = jnp.float32
MASK_FLOOR = -1e30
LOG2E = math.log2(math.e)
LN2 = math.log(2.0)
MIB = 1 << 20
QH = 256
CHUNK = 64
HBM = pl.BlockSpec(memory_space=pltpu.HBM)
VMEM = pl.BlockSpec(memory_space=pltpu.VMEM)
SMEM = pl.BlockSpec(memory_space=pltpu.SMEM)


def in_hbm(x):
    return pltpu.with_memory_space_constraint(x, pltpu.HBM)


def dot(a, b):
    return lax.dot_general(a, b, (((1,), (0,)), ((), ())), preferred_element_type=F32)


def dot_t(a, b):
    return lax.dot_general(a, b, (((1,), (1,)), ((), ())), preferred_element_type=F32)


def rms_normalize(values):
    stats = values.astype(F32)
    inv_rms = lax.rsqrt(jnp.mean(stats * stats, axis=-1, keepdims=True) + 1e-6)
    return (stats * inv_rms).astype(BF16)


def ds(start, size):
    return pl.ds(start if isinstance(start, int) else pl.multiple_of(start, size), size)


def gather_item(n, first_pair, pairs, block_len, item, k_hbm, v_hbm, kt, vt, sem, act):
    block = item // pairs
    pair = item - block * pairs
    rows = ds(block * block_len, block_len)
    for side, (src, dst) in enumerate(((k_hbm, kt), (v_hbm, vt))):
        copy = pltpu.make_async_copy(src.at[rows, first_pair + pair], dst.at[pair, rows], sem.at[side])
        copy.start() if act == 'start' else copy.wait()


def gather_range(lo, hi, n, pairs, block_len, first_pair, k_hbm, v_hbm, kt, vt, sem, act):
    lo = jnp.minimum(lo, n * pairs)
    hi = jnp.minimum(hi, n * pairs)

    @pl.loop(lo, hi)
    def _(item):
        gather_item(n, first_pair, pairs, block_len, item, k_hbm, v_hbm, kt, vt, sem, act)


def qkv_kernel(pairs, block_len, n_ref, x_hbm, wq_hbm, wkv_hbm, k_hbm, v_hbm, q_ref, kv_ref, kt, vt, x_ref, a_ref, wbuf, xsem, wsem, gsem):
    n = n_ref[0]
    x_copy = pltpu.make_async_copy(x_hbm, x_ref, xsem)
    x_copy.start()
    slots, _, tile = wbuf.shape
    q_steps = wq_hbm.shape[1] // tile
    kv_steps = wkv_hbm.shape[1] // tile
    steps = q_steps + kv_steps

    def fetch(step, slot):
        @pl.when(step < q_steps)
        def _():
            pltpu.make_async_copy(wq_hbm.at[:, ds(step * tile, tile)], wbuf.at[slot], wsem.at[slot]).start()

        @pl.when(step >= q_steps)
        def _():
            pltpu.make_async_copy(wkv_hbm.at[:, ds((step - q_steps) * tile, tile)], wbuf.at[slot], wsem.at[slot]).start()

    for step in range(slots - 1):
        fetch(step, step)
    x_copy.wait()
    a_ref[...] = rms_normalize(x_ref[...])
    share = (n * pairs + steps - 2) // (steps - 1)
    for out_ref, first, count in ((q_ref, 0, q_steps), (kv_ref, q_steps, kv_steps)):
        def body(i, carry):
            step = first + i
            slot = lax.rem(step, slots)
            ahead = step + slots - 1

            @pl.when(ahead < steps)
            def _():
                fetch(ahead, lax.rem(ahead, slots))

            gather_range(step * share, (step + 1) * share, n, pairs, block_len, 0, k_hbm, v_hbm, kt, vt, gsem, 'start')
            pltpu.make_async_copy(wq_hbm.at[:, 0:tile], wbuf.at[slot], wsem.at[slot]).wait()
            for at in range(0, tile, 512):
                out_ref[:, ds(i * tile + at, 512)] = dot(a_ref[...], wbuf[slot, :, at:at + 512]).astype(BF16)
            return carry

        lax.fori_loop(0, count, body, 0)
    gather_range(0, n * pairs, n, pairs, block_len, 0, k_hbm, v_hbm, kt, vt, gsem, 'wait')


def parity_max(x):
    x = jnp.maximum(x, pltpu.roll(x, 2, 0))
    return jnp.maximum(x, pltpu.roll(x, 4, 0))


def parity_sum(x):
    x = x + pltpu.roll(x, 2, 0)
    return x + pltpu.roll(x, 4, 0)


def fetch_gate_up(wg_hbm, wu_hbm, i, parts_ref, sems):
    half, tile = parts_ref.shape[0] // 2, parts_ref.shape[2]
    return [pltpu.make_async_copy(w.at[:, ds((i * half + j) * tile, tile)], parts_ref.at[side * half + j], sems.at[side * half + j])
            for j in range(half) for side, w in enumerate((wg_hbm, wu_hbm))]


def project_out(x_ref, o_refs, fetch_wo, wo_ref, h_ref, b_ref):
    width = h_ref.shape[1]
    steps = width // wo_ref.shape[2]

    def project(i, sq):
        cols = ds(i * 512, 512)
        slot = lax.rem(i, 2)
        fetch_wo(i, slot).wait()
        part = dot(jnp.concatenate([o[...] for o in o_refs], axis=1), wo_ref[slot])

        @pl.when(i + 2 < steps)
        def _():
            fetch_wo(i + 2, slot).start()

        h = (x_ref[:, cols].astype(F32) + part).astype(BF16)
        h_ref[:, cols] = h
        h = h.astype(F32)
        return sq + jnp.sum(h * h, axis=1, keepdims=True)

    sq = lax.fori_loop(0, steps, project, jnp.zeros((x_ref.shape[0], 1), F32))
    inv_rms = lax.rsqrt(sq * (1.0 / width) + 1e-6)
    b_ref[...] = (h_ref[...].astype(F32) * inv_rms).astype(BF16)


def attn_kernel(first_pair, gather_pairs, n_others, block_len, n_ref, q_ref, kv_ref, kt_ref, vt_ref, *rest):
    if gather_pairs:
        k_hbm, v_hbm, lse_ref, o_ref, kt_next, vt_next, *rest = rest
    else:
        others, rest = rest[:n_others], rest[n_others:]
        x_hbm, wo_hbm, wg_hbm, wu_hbm, lse_ref, h_ref, b_ref, gu_next, x_ref, wo_ref, o_ref, wo_sem, gu_sem, *rest = rest
    m_ref, l_ref, acc_ref, s_ref, p_ref, mx_ref, al_ref, gsem = rest
    n = n_ref[0]
    pairs = kt_ref.shape[0]
    scale = LOG2E * 128 ** -0.5
    keys = 2 * block_len
    if gather_pairs:
        gather_range(0, n * gather_pairs, n, gather_pairs, block_len, first_pair + pairs, k_hbm, v_hbm, kt_next, vt_next, gsem, 'start')
    else:
        def fetch_wo(i, slot):
            return pltpu.make_async_copy(wo_hbm.at[:, ds(i * 512, 512)], wo_ref.at[slot], wo_sem.at[slot])

        x_copy = pltpu.make_async_copy(x_hbm, x_ref, gsem.at[0])
        x_copy.start()
        fetch_wo(0, 0).start()
        fetch_wo(1, 1).start()
        ahead = fetch_gate_up(wg_hbm, wu_hbm, 0, gu_next, gu_sem)
        for copy in ahead:
            copy.start()

    def cols_of(p):
        return ds((first_pair + p) * 256, 256)

    def new_keys(p, carry):
        kn = kv_ref[:, cols_of(p)]
        vn = kv_ref[:, ds((first_pair + p) * 256 + q_ref.shape[1], 256)]
        state = [[None, None], [None, None]]
        for h in range(2):
            hs = slice(h * 128, h * 128 + 128)
            kh = kn[:, hs]
            vth = vn[:, hs].T
            for qh in range(2):
                rows = QH * (qh + 1)
                qb = q_ref[qh * QH:(qh + 1) * QH, cols_of(p)]
                s = dot_t(kh[:rows], qb[:, hs])
                key = lax.broadcasted_iota(jnp.int32, (QH, QH), 0)
                query = lax.broadcasted_iota(jnp.int32, (QH, QH), 1)
                tri = jnp.where(key <= query, s[rows - QH:], MASK_FLOOR)
                s = tri if qh == 0 else jnp.concatenate([s[:QH], tri], axis=0)
                m = jnp.max(s, axis=0, keepdims=True) * scale
                e = jnp.exp2(s * scale - m)
                state[qh][h] = (m, jnp.sum(e, axis=0, keepdims=True))
                acc_ref[p, qh, hs] = dot(vth[:, :rows], e.astype(BF16))
        even8 = lax.broadcasted_iota(jnp.int32, (8, QH), 0) % 2 == 0
        for qh in range(2):
            (m0, l0), (m1, l1) = state[qh]
            m_ref[p, qh] = jnp.where(even8, jnp.broadcast_to(m0, (8, QH)), jnp.broadcast_to(m1, (8, QH)))
            l_ref[p, qh] = jnp.where(even8, jnp.broadcast_to(l0, (8, QH)), jnp.broadcast_to(l1, (8, QH))) * 0.25
        return carry

    lax.fori_loop(0, pairs // 2, lambda i, c: new_keys(2 * i + 1, new_keys(2 * i, c)), 0)

    def parity_masks(axis):
        parity = lax.broadcasted_iota(jnp.int32, (16, 128), axis) % 2
        return [jnp.where(parity == h, 1.0, 0.0).astype(BF16)[None] for h in range(2)]

    def k_block(p, b):
        x3 = kt_ref[p, ds(b * keys, keys), :].reshape(keys // 16, 16, 128)
        return jnp.concatenate([(x3 * mask).reshape(keys, 128) for mask in parity_masks(0)], axis=1)

    def v_block(p, b):
        vx = vt_ref[p, ds(b * keys, keys), :].T
        tiles = [vx[:, c:c + 128].reshape(8, 16, 128) for c in range(0, keys, 128)]
        return jnp.concatenate([jnp.concatenate([(t * mask).reshape(128, 128) for t in tiles], axis=1) for mask in parity_masks(1)], axis=0)

    def scores(ke, p, qh):
        s = dot_t(ke, q_ref[qh * QH:(qh + 1) * QH, cols_of(p)])
        s_ref[qh] = s
        mx_ref[qh] = jnp.max(s.reshape(keys // 8, 8, QH), axis=0)

    def weights(p, qh):
        m_old = m_ref[p, qh]
        m = jnp.maximum(m_old, parity_max(mx_ref[qh]) * scale)
        alpha = jnp.exp2(m_old - m)
        total = l_ref[p, qh] * alpha
        for r in range(0, keys, CHUNK):
            s3 = s_ref[qh, r:r + CHUNK].reshape(CHUNK // 8, 8, QH)
            e = jnp.exp2(s3 * scale - m[None])
            total = total + jnp.sum(e, axis=0)
            p_ref[qh, r:r + CHUNK] = e.reshape(CHUNK, QH).astype(BF16)
        l_ref[p, qh] = total
        m_ref[p, qh] = m
        al_ref[qh] = alpha

    def values(ve, p, qh):
        out = dot(ve, p_ref[qh])
        alpha = al_ref[qh]
        acc_ref[p, qh, 0:128] = acc_ref[p, qh, 0:128] * alpha[0:1] + out[0:128]
        acc_ref[p, qh, 128:256] = acc_ref[p, qh, 128:256] * alpha[1:2] + out[128:256]

    def following(p, b):
        wrap = b + 1 == n
        return jnp.where(wrap, p + 1, p), jnp.where(wrap, 0, b + 1)

    def step(carry):
        older, now = carry
        nxt = following(*now)
        ve = v_block(*older)
        ke = k_block(*nxt)
        for qh in range(2):
            values(ve, older[0], qh)
            weights(now[0], qh)
            scores(ke, nxt[0], qh)
        return now, nxt

    @pl.when(n > 0)
    def _():
        first = (jnp.int32(0), jnp.int32(0))
        second = following(*first)
        ke = k_block(*first)
        for qh in range(2):
            scores(ke, 0, qh)
        ke = k_block(*second)
        for qh in range(2):
            weights(0, qh)
            scores(ke, second[0], qh)
        older, now = lax.fori_loop(0, (pairs * n - 2) // 2, lambda t, c: step(step(c)), (first, second))
        ve, ve_now = v_block(*older), v_block(*now)
        for qh in range(2):
            values(ve, older[0], qh)
            weights(now[0], qh)
            values(ve_now, now[0], qh)

    def finish(p, carry):
        for qh in range(2):
            l = parity_sum(l_ref[p, qh])
            lse_ref[p, :, qh * QH:(qh + 1) * QH] = ((m_ref[p, qh] + jnp.log2(l)) * LN2)[0:2]
            inv = 1.0 / l
            o = jnp.concatenate([acc_ref[p, qh, h * 128:(h + 1) * 128] * inv[h:h + 1] for h in range(2)], axis=0)
            o_ref[qh * QH:(qh + 1) * QH, ds(p * 256, 256)] = o.T.astype(BF16)
        return carry

    lax.fori_loop(0, pairs // 2, lambda i, c: finish(2 * i + 1, finish(2 * i, c)), 0)
    if gather_pairs:
        gather_range(0, n * gather_pairs, n, gather_pairs, block_len, first_pair + pairs, k_hbm, v_hbm, kt_next, vt_next, gsem, 'wait')
    else:
        x_copy.wait()
        for copy in ahead:
            copy.wait()
        project_out(x_ref, (*others, o_ref), fetch_wo, wo_ref, h_ref, b_ref)


def mlp_kernel(stages, h_ref, b_ref, gu_first, wg_hbm, wu_hbm, wd_hbm, y_ref, hid_ref, buf, g_ref, u_ref, ybuf, wsem, send_sem, recv_sem):
    me = lax.axis_index('pipe')
    right = lax.rem(me + 1, stages)
    left = lax.rem(me + stages - 1, stages)
    barrier = pltpu.get_barrier_semaphore()
    pl.semaphore_signal(barrier, inc=1, device_id={'pipe': left}, device_id_type=pl.DeviceIdType.MESH)
    slots, parts, depth, tile = buf.shape
    gu_cols = tile * parts // 2
    gu_steps = wg_hbm.shape[1] // gu_cols
    down_steps = wd_hbm.shape[1] // tile
    sub = g_ref.shape[1]
    subs = gu_cols // sub

    def fetch_gu(i, slot):
        return fetch_gate_up(wg_hbm, wu_hbm, i, buf.at[slot], wsem.at[slot])

    def fetch_down(i, slot):
        return [pltpu.make_async_copy(wd_hbm.at[pl.ds(j * depth, depth), ds(i * tile, tile)], buf.at[slot, j], wsem.at[slot, j]) for j in range(parts)]

    def start(copies):
        for c in copies:
            c.start()

    def act(g, u):
        return (g * jax.nn.sigmoid(g) * u).astype(BF16)

    for i in range(1, slots - 1):
        start(fetch_gu(i, i))

    def gate_up(i, first):
        slot = lax.rem(i, slots)
        ahead = i + slots - 1
        next_slot = lax.rem(ahead, slots)

        @pl.when(ahead < gu_steps)
        def _():
            start(fetch_gu(ahead, next_slot))

        @pl.when(ahead >= gu_steps)
        def _():
            start(fetch_down(ahead - gu_steps, next_slot))

        b = b_ref[...]
        w = gu_first if first else buf.at[slot]
        if not first:
            for c in fetch_gu(i, slot):
                c.wait()
            hid_ref[:, ds((subs * i - 1) * sub, sub)] = act(g_ref[...], u_ref[...])
        for k in range(subs):
            part, at = k * sub // tile, k * sub % tile
            g = dot(b, w[part, :, at:at + sub])
            u = dot(b, w[parts // 2 + part, :, at:at + sub])
            if k < subs - 1:
                hid_ref[:, ds((subs * i + k) * sub, sub)] = act(g, u)
            else:
                g_ref[...] = g
                u_ref[...] = u

    gate_up(0, True)

    @pl.loop(1, gu_steps)
    def _(i):
        gate_up(i, False)

    hid_ref[:, (subs * gu_steps - 1) * sub:] = act(g_ref[...], u_ref[...])

    rows = h_ref.shape[0] // 2

    def send(i, mh):
        cols = ds(i * tile, tile)
        part = pl.ds(mh * rows, rows)
        return pltpu.make_async_remote_copy(
            src_ref=ybuf.at[part, cols], dst_ref=y_ref.at[part, cols], send_sem=send_sem.at[i, mh],
            recv_sem=recv_sem.at[i, mh], device_id={'pipe': right}, device_id_type=pl.DeviceIdType.MESH)

    pl.semaphore_wait(barrier, 1)

    @pl.loop(0, down_steps)
    def _(i):
        slot = lax.rem(i + gu_steps, slots)

        @pl.when(i + slots - 1 < down_steps)
        def _():
            start(fetch_down(i + slots - 1, lax.rem(i + gu_steps + slots - 1, slots)))

        for c in fetch_down(i, slot):
            c.wait()
        cols = ds(i * tile, tile)
        for mh in range(2):
            part = slice(mh * rows, (mh + 1) * rows)
            out = h_ref[part, cols].astype(F32)
            for k in range(parts):
                out = out + dot(hid_ref[part, k * depth:(k + 1) * depth], buf[slot, k])
            ybuf[part, cols] = out.astype(BF16)
            send(i, mh).start()

    @pl.loop(0, down_steps)
    def _(i):
        for mh in range(2):
            send(i, mh).wait()


def params(limit_mib, **kwargs):
    return pltpu.CompilerParams(vmem_limit_bytes=limit_mib * MIB, **kwargs)


def solution(mesh):
    stages = mesh.shape['pipe']

    def device_step(x, slice_idx, k_cache, v_cache, w_q, w_kv, w_o, w_gate, w_up, w_down):
        seq, width = x.shape
        cache_len, n_heads, head_dim = k_cache.shape
        pairs = n_heads // 2
        x, w_q, w_kv, w_o, w_gate, w_up, w_down = map(in_hbm, (x, w_q[0], w_kv[0], w_o[0], w_gate[0], w_up[0], w_down[0]))
        ff = w_gate.shape[1]
        k4 = in_hbm(k_cache.reshape(cache_len, pairs, 2, head_dim))
        v4 = in_hbm(v_cache.reshape(cache_len, pairs, 2, head_dim))
        phases = (2, 2, 4)
        gathered = lambda count: [pltpu.VMEM((count, cache_len, 2, head_dim), BF16)] * 2
        big = lambda *shape: pltpu.VMEM(shape, BF16)
        dma = pltpu.SemaphoreType.DMA

        q, kv, kt, vt = pl.pallas_call(
            functools.partial(qkv_kernel, phases[0], seq), name='qkv',
            in_specs=[SMEM, HBM, HBM, HBM, HBM, HBM], out_specs=[VMEM] * 4,
            out_shape=[pltpu.VMEM((seq, width), BF16), pltpu.VMEM((seq, 2 * width), BF16)] + gathered(phases[0]),
            scratch_shapes=[big(seq, width), big(seq, width), big(3, width, 1024), dma, dma((3,)), dma((2,))],
            compiler_params=params(22),
        )(slice_idx, x, w_q, w_kv, k4, v4)

        outs, lses, first = [], [], 0
        for phase, count in enumerate(phases):
            last = phase == len(phases) - 1
            native = (count, 2 * cache_len, head_dim)
            lse_shape = jax.ShapeDtypeStruct((count, 2, seq), F32)
            mine = big(seq, count * 256)
            if last:
                extra = [big(seq, width), big(2, width, 512), mine, dma((2,)), dma((4,))]
                shapes = [lse_shape, big(seq, width), big(seq, width), big(4, width, 512)]
                more = (*outs, x, w_o, w_gate, w_up)
            else:
                extra = []
                shapes = [lse_shape, mine] + gathered(phases[phase + 1])
                more = (k4, v4)
            lse, *res = pl.pallas_call(
                functools.partial(attn_kernel, first, 0 if last else phases[phase + 1], len(outs) if last else 0, seq), name='attn',
                in_specs=[SMEM] + [VMEM] * (4 + (len(outs) if last else 0)) + [HBM] * (4 if last else 2), out_specs=[VMEM] * len(shapes), out_shape=shapes,
                scratch_shapes=extra + [pltpu.VMEM((count, 2, 8, QH), F32), pltpu.VMEM((count, 2, 8, QH), F32), pltpu.VMEM((count, 2, 256, QH), F32),
                                        pltpu.VMEM((2, 2 * seq, QH), F32), big(2, 2 * seq, QH),
                                        pltpu.VMEM((2, 8, QH), F32), pltpu.VMEM((2, 8, QH), F32), dma((2,))],
                compiler_params=params(17 if last else 9),
            )(slice_idx, q, kv, kt.reshape(native), vt.reshape(native), *more)
            lses.append(lse)
            first += count
            if last:
                h, b, gu_first = res
            else:
                o, kt, vt = res
                outs.append(o)
        lse = jnp.concatenate(lses).reshape(n_heads, seq).T

        y_next = pl.pallas_call(
            functools.partial(mlp_kernel, stages), name='mlp', in_specs=[VMEM] * 3 + [HBM] * 3, out_specs=HBM,
            out_shape=jax.ShapeDtypeStruct((seq, width), BF16),
            scratch_shapes=[big(seq, ff), big(2, 4, width, 512), pltpu.VMEM((seq, 256), F32), pltpu.VMEM((seq, 256), F32), big(seq, width),
                            dma((2, 4)), dma((4, 2)), dma((4, 2))],
            compiler_params=params(34, collective_id=0, has_side_effects=True),
        )(h, b, gu_first, w_gate, w_up, w_down)
        return y_next, lse

    rows_spec = P(('data', 'pipe'), None)
    cache_spec = P(('data', 'pipe'), None, None)
    stage_spec = P('pipe', None, None)
    return jax.shard_map(
        device_step,
        mesh=mesh,
        in_specs=(rows_spec, P(('data', 'pipe')), cache_spec, cache_spec) + (stage_spec,) * 6,
        out_specs=(rows_spec, rows_spec),
        check_vma=False,
    )
```

```python
import functools
import math

import jax
import jax.numpy as jnp
from jax import lax
from jax.experimental import pallas as pl
from jax.experimental.pallas import tpu as pltpu
from jax.sharding import PartitionSpec as P

BF16 = jnp.bfloat16
F32 = jnp.float32
MASK_FLOOR = -1e30
LOG2E = math.log2(math.e)
LN2 = math.log(2.0)
MIB = 1 << 20
QH = 256
CHUNK = 64
HBM = pl.BlockSpec(memory_space=pltpu.HBM)
VMEM = pl.BlockSpec(memory_space=pltpu.VMEM)
SMEM = pl.BlockSpec(memory_space=pltpu.SMEM)


def in_hbm(x):
    return pltpu.with_memory_space_constraint(x, pltpu.HBM)


def dot(a, b):
    return lax.dot_general(a, b, (((1,), (0,)), ((), ())), preferred_element_type=F32)


def dot_t(a, b):
    return lax.dot_general(a, b, (((1,), (1,)), ((), ())), preferred_element_type=F32)


def rms_normalize(values):
    stats = values.astype(F32)
    inv_rms = lax.rsqrt(jnp.mean(stats * stats, axis=-1, keepdims=True) + 1e-6)
    return (stats * inv_rms).astype(BF16)


def ds(start, size):
    return pl.ds(start if isinstance(start, int) else pl.multiple_of(start, size), size)


def gather_item(n, first_pair, pairs, block_len, item, k_hbm, v_hbm, kt, vt, sem, act):
    block = item // pairs
    pair = item - block * pairs
    rows = ds(block * block_len, block_len)
    for side, (src, dst) in enumerate(((k_hbm, kt), (v_hbm, vt))):
        copy = pltpu.make_async_copy(src.at[rows, first_pair + pair], dst.at[pair, rows], sem.at[side])
        copy.start() if act == 'start' else copy.wait()


def gather_range(lo, hi, n, pairs, block_len, first_pair, k_hbm, v_hbm, kt, vt, sem, act):
    lo = jnp.minimum(lo, n * pairs)
    hi = jnp.minimum(hi, n * pairs)

    @pl.loop(lo, hi)
    def _(item):
        gather_item(n, first_pair, pairs, block_len, item, k_hbm, v_hbm, kt, vt, sem, act)


def qkv_kernel(pairs, block_len, n_ref, x_hbm, wq_hbm, wkv_hbm, k_hbm, v_hbm, q_ref, kv_ref, kt, vt, x_ref, a_ref, wbuf, xsem, wsem, gsem):
    n = n_ref[0]
    x_copy = pltpu.make_async_copy(x_hbm, x_ref, xsem)
    x_copy.start()
    slots, _, tile = wbuf.shape
    q_steps = wq_hbm.shape[1] // tile
    kv_steps = wkv_hbm.shape[1] // tile
    steps = q_steps + kv_steps

    def fetch(step, slot):
        @pl.when(step < q_steps)
        def _():
            pltpu.make_async_copy(wq_hbm.at[:, ds(step * tile, tile)], wbuf.at[slot], wsem.at[slot]).start()

        @pl.when(step >= q_steps)
        def _():
            pltpu.make_async_copy(wkv_hbm.at[:, ds((step - q_steps) * tile, tile)], wbuf.at[slot], wsem.at[slot]).start()

    fetch(0, 0)
    x_copy.wait()
    for step in range(1, slots - 1):
        fetch(step, step)

    @pl.loop(0, x_ref.shape[0] // 32)
    def _(r):
        rows = ds(r * 32, 32)
        a_ref[rows, :] = rms_normalize(x_ref[rows, :])

    share = (n * pairs + steps - 2) // (steps - 1)
    for out_ref, first, count in ((q_ref, 0, q_steps), (kv_ref, q_steps, kv_steps)):
        def body(i, carry):
            step = first + i
            slot = lax.rem(step, slots)
            ahead = step + slots - 1

            @pl.when(ahead < steps)
            def _():
                fetch(ahead, lax.rem(ahead, slots))

            gather_range(step * share, (step + 1) * share, n, pairs, block_len, 0, k_hbm, v_hbm, kt, vt, gsem, 'start')
            pltpu.make_async_copy(wq_hbm.at[:, 0:tile], wbuf.at[slot], wsem.at[slot]).wait()
            for at in range(0, tile, 512):
                out_ref[:, ds(i * tile + at, 512)] = dot(a_ref[...], wbuf[slot, :, at:at + 512]).astype(BF16)
            return carry

        lax.fori_loop(0, count, body, 0)
    gather_range(0, n * pairs, n, pairs, block_len, 0, k_hbm, v_hbm, kt, vt, gsem, 'wait')


def parity_max(x):
    x = jnp.maximum(x, pltpu.roll(x, 2, 0))
    return jnp.maximum(x, pltpu.roll(x, 4, 0))


def parity_sum(x):
    x = x + pltpu.roll(x, 2, 0)
    return x + pltpu.roll(x, 4, 0)


def fetch_gate_up(wg_hbm, wu_hbm, i, parts, sems):
    half, tile = len(parts) // 2, parts[0].shape[1]
    return [pltpu.make_async_copy(w.at[:, ds((i * half + j) * tile, tile)], parts[side * half + j], sems.at[side * half + j])
            for j in range(half) for side, w in enumerate((wg_hbm, wu_hbm))]


def project_out(x_ref, o_refs, fetch_wo, wo_ref, h_ref, b_ref):
    width = h_ref.shape[1]
    steps = width // wo_ref.shape[2]

    def project(i, sq):
        cols = ds(i * 512, 512)
        slot = lax.rem(i, 2)
        fetch_wo(i, slot).wait()
        part = dot(jnp.concatenate([o[...] for o in o_refs], axis=1), wo_ref[slot])

        @pl.when(i + 2 < steps)
        def _():
            fetch_wo(i + 2, slot).start()

        h = (x_ref[:, cols].astype(F32) + part).astype(BF16)
        h_ref[:, cols] = h
        h = h.astype(F32)
        return sq + jnp.sum(h * h, axis=1, keepdims=True)

    sq = lax.fori_loop(0, steps, project, jnp.zeros((x_ref.shape[0], 1), F32))
    inv_rms = lax.rsqrt(sq * (1.0 / width) + 1e-6)
    for r in range(0, h_ref.shape[0], 64):
        b_ref[r:r + 64, :] = (h_ref[r:r + 64, :].astype(F32) * inv_rms[r:r + 64]).astype(BF16)


def attn_kernel(first_pair, gather_pairs, n_others, block_len, n_ref, q_ref, kv_ref, kt_ref, vt_ref, *rest):
    if gather_pairs:
        k_hbm, v_hbm, lse_ref, o_ref, kt_next, vt_next, *rest = rest
    else:
        others, other_lse, rest = rest[:n_others], rest[n_others:2 * n_others], rest[2 * n_others:]
        x_hbm, wo_hbm, wg_hbm, wu_hbm, lse_out, h_ref, b_ref, *rest = rest
        gu_next, (lse_ref, x_ref, wo_ref, o_ref, wo_sem, gu_sem, *rest) = rest[:4], rest[4:]
    m_ref, l_ref, acc_ref, s_ref, p_ref, mx_ref, al_ref, gsem = rest
    n = n_ref[0]
    pairs = kt_ref.shape[0]
    scale = LOG2E * 128 ** -0.5
    keys = 2 * block_len
    if gather_pairs:
        gather_range(0, n * gather_pairs, n, gather_pairs, block_len, first_pair + pairs, k_hbm, v_hbm, kt_next, vt_next, gsem, 'start')
    else:
        def fetch_wo(i, slot):
            return pltpu.make_async_copy(wo_hbm.at[:, ds(i * 512, 512)], wo_ref.at[slot], wo_sem.at[slot])

        x_copy = pltpu.make_async_copy(x_hbm, x_ref, gsem.at[0])
        x_copy.start()
        fetch_wo(0, 0).start()
        fetch_wo(1, 1).start()
        ahead = fetch_gate_up(wg_hbm, wu_hbm, 0, gu_next, gu_sem)
        for copy in ahead:
            copy.start()

    def cols_of(p):
        return ds((first_pair + p) * 256, 256)

    def new_keys(p_list):
        units = [(p, h, qh) for p in p_list for h in range(2) for qh in range(2)]
        key = lax.broadcasted_iota(jnp.int32, (QH, QH), 0)
        query = lax.broadcasted_iota(jnp.int32, (QH, QH), 1)
        visible = key <= query
        state, s_of, e_of = {}, {}, {}

        def cols_at(p, h, base=0):
            return ds(base + (first_pair + p) * 256 + h * 128, 128)

        def scores_new(u):
            p, h, qh = units[u]
            rows = QH * (qh + 1)
            s_of[u] = dot_t(kv_ref[:rows, cols_at(p, h)], q_ref[qh * QH:rows, cols_at(p, h)])

        def weights_new(u):
            p, h, qh = units[u]
            s = s_of.pop(u)
            parts = [s[:QH]] * qh + [jnp.where(visible, s[QH * qh:], MASK_FLOOR)]
            m = jnp.max(functools.reduce(jnp.maximum, parts), axis=0, keepdims=True) * scale
            es = [jnp.exp2(part * scale - m) for part in parts]
            state[u] = (m, jnp.sum(functools.reduce(jnp.add, es), axis=0, keepdims=True))
            e_of[u] = jnp.concatenate([e.astype(BF16) for e in es], axis=0)

        def values_new(u):
            p, h, qh = units[u]
            vt = kv_ref[:QH * (qh + 1), cols_at(p, h, q_ref.shape[1])].T
            acc_ref[p, qh, h * 128:h * 128 + 128] = dot(vt, e_of.pop(u))

        scores_new(0)
        for u in range(len(units)):
            if u + 1 < len(units):
                scores_new(u + 1)
            weights_new(u)
            if u > 0:
                values_new(u - 1)
        values_new(len(units) - 1)
        even8 = lax.broadcasted_iota(jnp.int32, (8, QH), 0) % 2 == 0
        for u, (p, h, qh) in enumerate(units):
            if h == 0:
                (m0, l0), (m1, l1) = state[u], state[u + 2]
                m_ref[p, qh] = jnp.where(even8, jnp.broadcast_to(m0, (8, QH)), jnp.broadcast_to(m1, (8, QH)))
                l_ref[p, qh] = jnp.where(even8, jnp.broadcast_to(l0, (8, QH)), jnp.broadcast_to(l1, (8, QH))) * 0.25

    @pl.loop(0, pairs // 2)
    def _(i):
        new_keys([2 * i, 2 * i + 1])

    def parity_masks(axis):
        parity = lax.broadcasted_iota(jnp.int32, (16, 128), axis) % 2
        return [jnp.where(parity == h, 1.0, 0.0).astype(BF16)[None] for h in range(2)]

    def k_block(p, b):
        x3 = kt_ref[p, ds(b * keys, keys), :].reshape(keys // 16, 16, 128)
        return jnp.concatenate([(x3 * mask).reshape(keys, 128) for mask in parity_masks(0)], axis=1)

    def v_block(p, b):
        vx = vt_ref[p, ds(b * keys, keys), :].T
        tiles = [vx[:, c:c + 128].reshape(8, 16, 128) for c in range(0, keys, 128)]
        return jnp.concatenate([jnp.concatenate([(t * mask).reshape(128, 128) for t in tiles], axis=1) for mask in parity_masks(1)], axis=0)

    def scores(ke, p, qh):
        s = dot_t(ke, q_ref[qh * QH:(qh + 1) * QH, cols_of(p)])
        s_ref[qh] = s
        mx_ref[qh] = jnp.max(s.reshape(keys // 8, 8, QH), axis=0)

    def weights(p, qh):
        m_old = m_ref[p, qh]
        m = jnp.maximum(m_old, parity_max(mx_ref[qh]) * scale)
        alpha = jnp.exp2(m_old - m)
        total = l_ref[p, qh] * alpha
        for r in range(0, keys, CHUNK):
            s3 = s_ref[qh, r:r + CHUNK].reshape(CHUNK // 8, 8, QH)
            e = jnp.exp2(s3 * scale - m[None])
            total = total + jnp.sum(e, axis=0)
            p_ref[qh, r:r + CHUNK] = e.reshape(CHUNK, QH).astype(BF16)
        l_ref[p, qh] = total
        m_ref[p, qh] = m
        al_ref[qh] = alpha

    def values(ve, p, qh):
        out = dot(ve, p_ref[qh])
        alpha = al_ref[qh]
        acc_ref[p, qh, 0:128] = acc_ref[p, qh, 0:128] * alpha[0:1] + out[0:128]
        acc_ref[p, qh, 128:256] = acc_ref[p, qh, 128:256] * alpha[1:2] + out[128:256]

    def following(p, b):
        wrap = b + 1 == n
        return jnp.where(wrap, p + 1, p), jnp.where(wrap, 0, b + 1)

    def step(carry):
        older, now = carry
        nxt = following(*now)
        ve = v_block(*older)
        ke = k_block(*nxt)
        for qh in range(2):
            values(ve, older[0], qh)
            weights(now[0], qh)
            scores(ke, nxt[0], qh)
        return now, nxt

    @pl.when(n > 0)
    def _():
        first = (jnp.int32(0), jnp.int32(0))
        second = following(*first)
        ke = k_block(*first)
        for qh in range(2):
            scores(ke, 0, qh)
        ke = k_block(*second)
        for qh in range(2):
            weights(0, qh)
            scores(ke, second[0], qh)
        carry = (first, second)
        if pairs % 4 == 0:
            carry = lax.fori_loop(0, n - 1, lambda t, c: step(step(step(step(c)))), carry)
            older, now = step(step(carry))
        else:
            older, now = lax.fori_loop(0, (pairs * n - 2) // 2, lambda t, c: step(step(c)), carry)
        ve, ve_now = v_block(*older), v_block(*now)
        for qh in range(2):
            values(ve, older[0], qh)
            weights(now[0], qh)
            values(ve_now, now[0], qh)

    def finish(p, carry):
        for qh in range(2):
            l = parity_sum(l_ref[p, qh])
            lse_ref[p, :, qh * QH:(qh + 1) * QH] = ((m_ref[p, qh] + jnp.log2(l)) * LN2)[0:2]
            inv = 1.0 / l
            o = jnp.concatenate([acc_ref[p, qh, h * 128:(h + 1) * 128] * inv[h:h + 1] for h in range(2)], axis=0)
            o_ref[qh * QH:(qh + 1) * QH, ds(p * 256, 256)] = o.T.astype(BF16)
        return carry

    lax.fori_loop(0, pairs // 2, lambda i, c: finish(2 * i + 1, finish(2 * i, c)), 0)
    if gather_pairs:
        gather_range(0, n * gather_pairs, n, gather_pairs, block_len, first_pair + pairs, k_hbm, v_hbm, kt_next, vt_next, gsem, 'wait')
    else:
        row = 0
        for ref in (*other_lse, lse_ref):
            for p in range(ref.shape[0]):
                lse_out[row:row + 2, :] = ref[p]
                row += 2
        x_copy.wait()
        for copy in ahead:
            copy.wait()
        project_out(x_ref, (*others, o_ref), fetch_wo, wo_ref, h_ref, b_ref)


def mlp_kernel(stages, h_ref, b_ref, gu0, gu1, gu2, gu3, wg_hbm, wu_hbm, wd_hbm, y_ref, hid_ref, buf, g_ref, u_ref, ybuf, wsem, send_sem, recv_sem):
    me = lax.axis_index('pipe')
    right = lax.rem(me + 1, stages)
    left = lax.rem(me + stages - 1, stages)
    barrier = pltpu.get_barrier_semaphore()
    pl.semaphore_signal(barrier, inc=1, device_id={'pipe': left}, device_id_type=pl.DeviceIdType.MESH)
    slots, parts, depth, tile = buf.shape
    gu_cols = tile * parts // 2
    gu_steps = wg_hbm.shape[1] // gu_cols
    down_steps = wd_hbm.shape[1] // tile
    sub = g_ref.shape[1]
    subs = gu_cols // sub

    def fetch_gu(i, slot):
        return fetch_gate_up(wg_hbm, wu_hbm, i, [buf.at[slot, j] for j in range(parts)], wsem.at[slot])

    def fetch_down(i, slot):
        return [pltpu.make_async_copy(wd_hbm.at[pl.ds(j * depth, depth), ds(i * tile, tile)], buf.at[slot, j], wsem.at[slot, j]) for j in range(parts)]

    def start(copies):
        for c in copies:
            c.start()

    def act(g, u):
        return (g * jax.nn.sigmoid(g) * u).astype(BF16)

    for i in range(1, slots - 1):
        start(fetch_gu(i, i))

    def gate_up(i, first):
        slot = lax.rem(i, slots)
        ahead = i + slots - 1
        next_slot = lax.rem(ahead, slots)

        @pl.when(ahead < gu_steps)
        def _():
            start(fetch_gu(ahead, next_slot))

        @pl.when(ahead >= gu_steps)
        def _():
            start(fetch_down(ahead - gu_steps, next_slot))

        b = b_ref[...]
        w = (gu0, gu1, gu2, gu3) if first else [buf.at[slot, j] for j in range(parts)]
        if not first:
            for c in fetch_gu(i, slot):
                c.wait()
            hid_ref[:, ds((subs * i - 1) * sub, sub)] = act(g_ref[...], u_ref[...])
        for k in range(subs):
            part, at = k * sub // tile, k * sub % tile
            g = dot(b, w[part][:, at:at + sub])
            u = dot(b, w[parts // 2 + part][:, at:at + sub])
            if k < subs - 1:
                hid_ref[:, ds((subs * i + k) * sub, sub)] = act(g, u)
            else:
                g_ref[...] = g
                u_ref[...] = u

    gate_up(0, True)

    @pl.loop(1, gu_steps)
    def _(i):
        gate_up(i, False)

    hid_ref[:, (subs * gu_steps - 1) * sub:] = act(g_ref[...], u_ref[...])

    rows = h_ref.shape[0] // 2

    def send(i, mh):
        cols = ds(i * tile, tile)
        part = pl.ds(mh * rows, rows)
        return pltpu.make_async_remote_copy(
            src_ref=ybuf.at[part, cols], dst_ref=y_ref.at[part, cols], send_sem=send_sem.at[i, mh],
            recv_sem=recv_sem.at[i, mh], device_id={'pipe': right}, device_id_type=pl.DeviceIdType.MESH)

    pl.semaphore_wait(barrier, 1)

    @pl.loop(0, down_steps)
    def _(i):
        slot = lax.rem(i + gu_steps, slots)

        @pl.when(i + slots - 1 < down_steps)
        def _():
            start(fetch_down(i + slots - 1, lax.rem(i + gu_steps + slots - 1, slots)))

        for c in fetch_down(i, slot):
            c.wait()
        cols = ds(i * tile, tile)
        for mh in range(2):
            part = slice(mh * rows, (mh + 1) * rows)
            out = h_ref[part, cols].astype(F32)
            for k in range(parts):
                out = out + dot(hid_ref[part, k * depth:(k + 1) * depth], buf[slot, k])
            ybuf[part, cols] = out.astype(BF16)
            send(i, mh).start()

    @pl.loop(0, down_steps)
    def _(i):
        for mh in range(2):
            send(i, mh).wait()


def params(limit_mib, **kwargs):
    return pltpu.CompilerParams(vmem_limit_bytes=limit_mib * MIB, **kwargs)


def solution(mesh):
    stages = mesh.shape['pipe']

    def device_step(x, slice_idx, k_cache, v_cache, w_q, w_kv, w_o, w_gate, w_up, w_down):
        seq, width = x.shape
        cache_len, n_heads, head_dim = k_cache.shape
        pairs = n_heads // 2
        x, w_q, w_kv, w_o, w_gate, w_up, w_down = map(in_hbm, (x, w_q[0], w_kv[0], w_o[0], w_gate[0], w_up[0], w_down[0]))
        ff = w_gate.shape[1]
        k4 = in_hbm(k_cache.reshape(cache_len, pairs, 2, head_dim))
        v4 = in_hbm(v_cache.reshape(cache_len, pairs, 2, head_dim))
        phases = (2, 2, 4)
        gathered = lambda count: [pltpu.VMEM((count, cache_len, 2, head_dim), BF16)] * 2
        big = lambda *shape: pltpu.VMEM(shape, BF16)
        dma = pltpu.SemaphoreType.DMA

        q, kv, kt, vt = pl.pallas_call(
            functools.partial(qkv_kernel, phases[0], seq), name='qkv',
            in_specs=[SMEM, HBM, HBM, HBM, HBM, HBM], out_specs=[VMEM] * 4,
            out_shape=[pltpu.VMEM((seq, width), BF16), pltpu.VMEM((seq, 2 * width), BF16)] + gathered(phases[0]),
            scratch_shapes=[big(seq, width), big(seq, width), big(3, width, 1024), dma, dma((3,)), dma((2,))],
            compiler_params=params(18),
        )(slice_idx, x, w_q, w_kv, k4, v4)

        outs, lses, first = [], [], 0
        for phase, count in enumerate(phases):
            last = phase == len(phases) - 1
            native = (count, 2 * cache_len, head_dim)
            lse_shape = pltpu.VMEM((count, 2, seq), F32)
            mine = big(seq, count * 256)
            if last:
                extra = [lse_shape, big(seq, width), big(2, width, 512), mine, dma((2,)), dma((4,))]
                shapes = [jax.ShapeDtypeStruct((n_heads, seq), F32), big(seq, width), big(seq, width)] + [big(width, 512)] * 4
                more = (*outs, *lses, x, w_o, w_gate, w_up)
            else:
                extra = []
                shapes = [lse_shape, mine] + gathered(phases[phase + 1])
                more = (k4, v4)
            lse, *res = pl.pallas_call(
                functools.partial(attn_kernel, first, 0 if last else phases[phase + 1], len(outs) if last else 0, seq), name='attn',
                in_specs=[SMEM] + [VMEM] * (4 + (2 * len(outs) if last else 0)) + [HBM] * (4 if last else 2), out_specs=[VMEM] * len(shapes), out_shape=shapes,
                scratch_shapes=extra + [pltpu.VMEM((count, 2, 8, QH), F32), pltpu.VMEM((count, 2, 8, QH), F32), pltpu.VMEM((count, 2, 256, QH), F32),
                                        pltpu.VMEM((2, 2 * seq, QH), F32), big(2, 2 * seq, QH),
                                        pltpu.VMEM((2, 8, QH), F32), pltpu.VMEM((2, 8, QH), F32), dma((2,))],
                compiler_params=params(17 if last else 9),
            )(slice_idx, q, kv, kt.reshape(native), vt.reshape(native), *more)
            lses.append(lse)
            first += count
            if last:
                h, b, *gu_first = res
            else:
                o, kt, vt = res
                outs.append(o)
        y_next = pl.pallas_call(
            functools.partial(mlp_kernel, stages), name='mlp', in_specs=[VMEM] * 6 + [HBM] * 3, out_specs=HBM,
            out_shape=jax.ShapeDtypeStruct((seq, width), BF16),
            scratch_shapes=[big(seq, ff), big(2, 4, width, 512), pltpu.VMEM((seq, 256), F32), pltpu.VMEM((seq, 256), F32), big(seq, width),
                            dma((2, 4)), dma((4, 2)), dma((4, 2))],
            compiler_params=params(34, collective_id=0, has_side_effects=True),
        )(h, b, *gu_first, w_gate, w_up, w_down)
        return y_next, lse.T

    rows_spec = P(('data', 'pipe'), None)
    cache_spec = P(('data', 'pipe'), None, None)
    stage_spec = P('pipe', None, None)
    return jax.shard_map(
        device_step,
        mesh=mesh,
        in_specs=(rows_spec, P(('data', 'pipe')), cache_spec, cache_spec) + (stage_spec,) * 6,
        out_specs=(rows_spec, rows_spec),
        check_vma=False,
    )
```

```python
import functools
import math

import jax
import jax.numpy as jnp
from jax import lax
from jax.experimental import pallas as pl
from jax.experimental.pallas import tpu as pltpu
from jax.sharding import PartitionSpec as P

BF16 = jnp.bfloat16
F32 = jnp.float32
MASK_FLOOR = -1e30
LOG2E = math.log2(math.e)
LN2 = math.log(2.0)
MIB = 1 << 20
QH = 256
CHUNK = 64
HBM = pl.BlockSpec(memory_space=pltpu.HBM)
VMEM = pl.BlockSpec(memory_space=pltpu.VMEM)
SMEM = pl.BlockSpec(memory_space=pltpu.SMEM)


def in_hbm(x):
    return pltpu.with_memory_space_constraint(x, pltpu.HBM)


def dot(a, b):
    return lax.dot_general(a, b, (((1,), (0,)), ((), ())), preferred_element_type=F32)


def dot_t(a, b):
    return lax.dot_general(a, b, (((1,), (1,)), ((), ())), preferred_element_type=F32)


def rms_normalize(values):
    stats = values.astype(F32)
    inv_rms = lax.rsqrt(jnp.mean(stats * stats, axis=-1, keepdims=True) + 1e-6)
    return (stats * inv_rms).astype(BF16)


def ds(start, size):
    return pl.ds(start if isinstance(start, int) else pl.multiple_of(start, size), size)


def gather_item(n, first_pair, pairs, block_len, item, k_hbm, v_hbm, kt, vt, sem, act):
    block = item // pairs
    pair = item - block * pairs
    rows = ds(block * block_len, block_len)
    for side, (src, dst) in enumerate(((k_hbm, kt), (v_hbm, vt))):
        copy = pltpu.make_async_copy(src.at[rows, first_pair + pair], dst.at[pair, rows], sem.at[side])
        copy.start() if act == 'start' else copy.wait()


def gather_range(lo, hi, n, pairs, block_len, first_pair, k_hbm, v_hbm, kt, vt, sem, act):
    lo = jnp.minimum(lo, n * pairs)
    hi = jnp.minimum(hi, n * pairs)

    @pl.loop(lo, hi)
    def _(item):
        gather_item(n, first_pair, pairs, block_len, item, k_hbm, v_hbm, kt, vt, sem, act)


def qkv_kernel(pairs, block_len, n_ref, x_hbm, wq_hbm, wkv_hbm, k_hbm, v_hbm, q_ref, kv_ref, kt, vt, x_ref, a_ref, wbuf, xsem, wsem, gsem):
    n = n_ref[0]
    x_copy = pltpu.make_async_copy(x_hbm, x_ref, xsem)
    x_copy.start()
    slots, _, tile = wbuf.shape
    q_steps = wq_hbm.shape[1] // tile
    kv_steps = wkv_hbm.shape[1] // tile
    steps = q_steps + kv_steps

    def fetch(step, slot):
        @pl.when(step < q_steps)
        def _():
            pltpu.make_async_copy(wq_hbm.at[:, ds(step * tile, tile)], wbuf.at[slot], wsem.at[slot]).start()

        @pl.when(step >= q_steps)
        def _():
            pltpu.make_async_copy(wkv_hbm.at[:, ds((step - q_steps) * tile, tile)], wbuf.at[slot], wsem.at[slot]).start()

    fetch(0, 0)
    x_copy.wait()
    for step in range(1, slots - 1):
        fetch(step, step)

    @pl.loop(0, x_ref.shape[0] // 32)
    def _(r):
        rows = ds(r * 32, 32)
        a_ref[rows, :] = rms_normalize(x_ref[rows, :])

    share = (n * pairs + steps - 2) // (steps - 1)
    for out_ref, first, count in ((q_ref, 0, q_steps), (kv_ref, q_steps, kv_steps)):
        def body(i, carry):
            step = first + i
            slot = lax.rem(step, slots)
            ahead = step + slots - 1

            @pl.when(ahead < steps)
            def _():
                fetch(ahead, lax.rem(ahead, slots))

            gather_range(step * share, (step + 1) * share, n, pairs, block_len, 0, k_hbm, v_hbm, kt, vt, gsem, 'start')
            pltpu.make_async_copy(wq_hbm.at[:, 0:tile], wbuf.at[slot], wsem.at[slot]).wait()
            for at in range(0, tile, 512):
                out_ref[:, ds(i * tile + at, 512)] = dot(a_ref[...], wbuf[slot, :, at:at + 512]).astype(BF16)
            return carry

        lax.fori_loop(0, count, body, 0)
    gather_range(0, n * pairs, n, pairs, block_len, 0, k_hbm, v_hbm, kt, vt, gsem, 'wait')


def parity_max(x):
    x = jnp.maximum(x, pltpu.roll(x, 2, 0))
    return jnp.maximum(x, pltpu.roll(x, 4, 0))


def parity_sum(x):
    x = x + pltpu.roll(x, 2, 0)
    return x + pltpu.roll(x, 4, 0)


def fetch_gate_up(wg_hbm, wu_hbm, i, parts, sems):
    half, tile = len(parts) // 2, parts[0].shape[1]
    return [pltpu.make_async_copy(w.at[:, ds((i * half + j) * tile, tile)], parts[side * half + j], sems.at[side * half + j])
            for j in range(half) for side, w in enumerate((wg_hbm, wu_hbm))]


def project_out(x_ref, o_refs, fetch_wo, wo_ref, h_ref, b_ref):
    width = h_ref.shape[1]
    steps = width // wo_ref.shape[2]

    def project(i, sq):
        cols = ds(i * 512, 512)
        slot = lax.rem(i, 2)
        fetch_wo(i, slot).wait()
        part = dot(jnp.concatenate([o[...] for o in o_refs], axis=1), wo_ref[slot])

        @pl.when(i + 2 < steps)
        def _():
            fetch_wo(i + 2, slot).start()

        h = (x_ref[:, cols].astype(F32) + part).astype(BF16)
        h_ref[:, cols] = h
        h = h.astype(F32)
        return sq + jnp.sum(h * h, axis=1, keepdims=True)

    sq = lax.fori_loop(0, steps, project, jnp.zeros((x_ref.shape[0], 1), F32))
    inv_rms = lax.rsqrt(sq * (1.0 / width) + 1e-6)
    for r in range(0, h_ref.shape[0], 64):
        b_ref[r:r + 64, :] = (h_ref[r:r + 64, :].astype(F32) * inv_rms[r:r + 64]).astype(BF16)


def attn_kernel(first_pair, gather_pairs, n_others, block_len, n_ref, q_ref, kv_ref, kt_ref, vt_ref, *rest):
    if gather_pairs:
        k_hbm, v_hbm, lse_ref, o_ref, kt_next, vt_next, *rest = rest
    else:
        others, other_lse, rest = rest[:n_others], rest[n_others:2 * n_others], rest[2 * n_others:]
        x_hbm, wo_hbm, wg_hbm, wu_hbm, lse_out, h_ref, b_ref, *rest = rest
        gu_next, (lse_ref, x_ref, wo_ref, o_ref, wo_sem, gu_sem, *rest) = rest[:4], rest[4:]
    m_ref, l_ref, acc_ref, s_ref, p_ref, mx_ref, al_ref, gsem = rest
    n = n_ref[0]
    pairs = kt_ref.shape[0]
    scale = LOG2E * 128 ** -0.5
    keys = 2 * block_len
    if gather_pairs:
        gather_range(0, n * gather_pairs, n, gather_pairs, block_len, first_pair + pairs, k_hbm, v_hbm, kt_next, vt_next, gsem, 'start')
    else:
        def fetch_wo(i, slot):
            return pltpu.make_async_copy(wo_hbm.at[:, ds(i * 512, 512)], wo_ref.at[slot], wo_sem.at[slot])

        x_copy = pltpu.make_async_copy(x_hbm, x_ref, gsem.at[0])
        x_copy.start()
        fetch_wo(0, 0).start()
        fetch_wo(1, 1).start()
        ahead = fetch_gate_up(wg_hbm, wu_hbm, 0, gu_next, gu_sem)
        for copy in ahead:
            copy.start()

    def cols_of(p):
        return ds((first_pair + p) * 256, 256)

    def new_keys(p_list):
        units = [(p, h, qh) for p in p_list for h in range(2) for qh in range(2)]
        key = lax.broadcasted_iota(jnp.int32, (QH, QH), 0)
        query = lax.broadcasted_iota(jnp.int32, (QH, QH), 1)
        visible = key <= query
        state, s_of, e_of = {}, {}, {}

        def cols_at(p, h, base=0):
            return ds(base + (first_pair + p) * 256 + h * 128, 128)

        def scores_new(u):
            p, h, qh = units[u]
            rows = QH * (qh + 1)
            s_of[u] = dot_t(kv_ref[:rows, cols_at(p, h)], q_ref[qh * QH:rows, cols_at(p, h)])

        def weights_new(u):
            p, h, qh = units[u]
            s = s_of.pop(u)
            parts = [s[:QH]] * qh + [jnp.where(visible, s[QH * qh:], MASK_FLOOR)]
            m = jnp.max(functools.reduce(jnp.maximum, parts), axis=0, keepdims=True) * scale
            es = [jnp.exp2(part * scale - m) for part in parts]
            state[u] = (m, jnp.sum(functools.reduce(jnp.add, es), axis=0, keepdims=True))
            e_of[u] = jnp.concatenate([e.astype(BF16) for e in es], axis=0)

        def values_new(u):
            p, h, qh = units[u]
            vt = kv_ref[:QH * (qh + 1), cols_at(p, h, q_ref.shape[1])].T
            acc_ref[p, qh, h * 128:h * 128 + 128] = dot(vt, e_of.pop(u))

        scores_new(0)
        for u in range(len(units)):
            if u + 1 < len(units):
                scores_new(u + 1)
            weights_new(u)
            if u > 0:
                values_new(u - 1)
        values_new(len(units) - 1)
        even8 = lax.broadcasted_iota(jnp.int32, (8, QH), 0) % 2 == 0
        for u, (p, h, qh) in enumerate(units):
            if h == 0:
                (m0, l0), (m1, l1) = state[u], state[u + 2]
                m_ref[p, qh] = jnp.where(even8, jnp.broadcast_to(m0, (8, QH)), jnp.broadcast_to(m1, (8, QH)))
                l_ref[p, qh] = jnp.where(even8, jnp.broadcast_to(l0, (8, QH)), jnp.broadcast_to(l1, (8, QH))) * 0.25

    @pl.loop(0, pairs // 2)
    def _(i):
        new_keys([2 * i, 2 * i + 1])

    def parity_masks(axis):
        parity = lax.broadcasted_iota(jnp.int32, (16, 128), axis) % 2
        return [jnp.where(parity == h, 1.0, 0.0).astype(BF16)[None] for h in range(2)]

    def k_block(p, b):
        x3 = kt_ref[p, ds(b * keys, keys), :].reshape(keys // 16, 16, 128)
        return jnp.concatenate([(x3 * mask).reshape(keys, 128) for mask in parity_masks(0)], axis=1)

    def v_block(p, b):
        vx = vt_ref[p, ds(b * keys, keys), :].T
        tiles = [vx[:, c:c + 128].reshape(8, 16, 128) for c in range(0, keys, 128)]
        return jnp.concatenate([jnp.concatenate([(t * mask).reshape(128, 128) for t in tiles], axis=1) for mask in parity_masks(1)], axis=0)

    def scores(ke, p, qh):
        s = dot_t(ke, q_ref[qh * QH:(qh + 1) * QH, cols_of(p)])
        s_ref[qh] = s
        mx_ref[qh] = jnp.max(s.reshape(keys // 8, 8, QH), axis=0)

    def weights(p, qh):
        m_old = m_ref[p, qh]
        m = jnp.maximum(m_old, parity_max(mx_ref[qh]) * scale)
        alpha = jnp.exp2(m_old - m)
        total = l_ref[p, qh] * alpha
        for r in range(0, keys, CHUNK):
            s3 = s_ref[qh, r:r + CHUNK].reshape(CHUNK // 8, 8, QH)
            e = jnp.exp2(s3 * scale - m[None])
            total = total + jnp.sum(e, axis=0)
            p_ref[qh, r:r + CHUNK] = e.reshape(CHUNK, QH).astype(BF16)
        l_ref[p, qh] = total
        m_ref[p, qh] = m
        al_ref[qh] = alpha

    def values(ve, p, qh):
        out = dot(ve, p_ref[qh])
        alpha = al_ref[qh]
        acc_ref[p, qh, 0:128] = acc_ref[p, qh, 0:128] * alpha[0:1] + out[0:128]
        acc_ref[p, qh, 128:256] = acc_ref[p, qh, 128:256] * alpha[1:2] + out[128:256]

    def following(p, b):
        wrap = b + 1 == n
        return jnp.where(wrap, p + 1, p), jnp.where(wrap, 0, b + 1)

    def step(carry):
        older, now = carry
        nxt = following(*now)
        ve = v_block(*older)
        ke = k_block(*nxt)
        for qh in range(2):
            values(ve, older[0], qh)
            weights(now[0], qh)
            scores(ke, nxt[0], qh)
        return now, nxt

    @pl.when(n > 0)
    def _():
        first = (jnp.int32(0), jnp.int32(0))
        second = following(*first)
        ke = k_block(*first)
        for qh in range(2):
            scores(ke, 0, qh)
        ke = k_block(*second)
        for qh in range(2):
            weights(0, qh)
            scores(ke, second[0], qh)
        steps = pairs * n - 2
        carry = lax.fori_loop(0, steps // 4, lambda t, c: step(step(step(step(c)))), (first, second))
        older, now = lax.fori_loop(0, lax.rem(steps, 4) // 2, lambda t, c: step(step(c)), carry)
        ve, ve_now = v_block(*older), v_block(*now)
        for qh in range(2):
            values(ve, older[0], qh)
            weights(now[0], qh)
            values(ve_now, now[0], qh)

    def finish(p, carry):
        for qh in range(2):
            l = parity_sum(l_ref[p, qh])
            lse_ref[p, :, qh * QH:(qh + 1) * QH] = ((m_ref[p, qh] + jnp.log2(l)) * LN2)[0:2]
            inv = 1.0 / l
            o = jnp.concatenate([acc_ref[p, qh, h * 128:(h + 1) * 128] * inv[h:h + 1] for h in range(2)], axis=0)
            o_ref[qh * QH:(qh + 1) * QH, ds(p * 256, 256)] = o.T.astype(BF16)
        return carry

    lax.fori_loop(0, pairs // 2, lambda i, c: finish(2 * i + 1, finish(2 * i, c)), 0)
    if gather_pairs:
        gather_range(0, n * gather_pairs, n, gather_pairs, block_len, first_pair + pairs, k_hbm, v_hbm, kt_next, vt_next, gsem, 'wait')
    else:
        row = 0
        for ref in (*other_lse, lse_ref):
            for p in range(ref.shape[0]):
                lse_out[row:row + 2, :] = ref[p]
                row += 2
        x_copy.wait()
        for copy in ahead:
            copy.wait()
        project_out(x_ref, (*others, o_ref), fetch_wo, wo_ref, h_ref, b_ref)


def mlp_kernel(stages, h_ref, b_ref, gu0, gu1, gu2, gu3, wg_hbm, wu_hbm, wd_hbm, y_ref, hid_ref, buf, g_ref, u_ref, ybuf, wsem, send_sem, recv_sem):
    me = lax.axis_index('pipe')
    right = lax.rem(me + 1, stages)
    left = lax.rem(me + stages - 1, stages)
    barrier = pltpu.get_barrier_semaphore()
    pl.semaphore_signal(barrier, inc=1, device_id={'pipe': left}, device_id_type=pl.DeviceIdType.MESH)
    slots, parts, depth, tile = buf.shape
    gu_cols = tile * parts // 2
    gu_steps = wg_hbm.shape[1] // gu_cols
    down_steps = wd_hbm.shape[1] // tile
    sub = g_ref.shape[1]
    subs = gu_cols // sub

    def fetch_gu(i, slot):
        return fetch_gate_up(wg_hbm, wu_hbm, i, [buf.at[slot, j] for j in range(parts)], wsem.at[slot])

    def fetch_down(i, slot):
        return [pltpu.make_async_copy(wd_hbm.at[pl.ds(j * depth, depth), ds(i * tile, tile)], buf.at[slot, j], wsem.at[slot, j]) for j in range(parts)]

    def start(copies):
        for c in copies:
            c.start()

    def act(g, u):
        return (g * jax.nn.sigmoid(g) * u).astype(BF16)

    for i in range(1, slots - 1):
        start(fetch_gu(i, i))

    def gate_up(i, first):
        slot = lax.rem(i, slots)
        ahead = i + slots - 1
        next_slot = lax.rem(ahead, slots)

        @pl.when(ahead < gu_steps)
        def _():
            start(fetch_gu(ahead, next_slot))

        @pl.when(ahead >= gu_steps)
        def _():
            start(fetch_down(ahead - gu_steps, next_slot))

        b = b_ref[...]
        w = (gu0, gu1, gu2, gu3) if first else [buf.at[slot, j] for j in range(parts)]
        if not first:
            for c in fetch_gu(i, slot):
                c.wait()
            hid_ref[:, ds((subs * i - 1) * sub, sub)] = act(g_ref[...], u_ref[...])
        for k in range(subs):
            part, at = k * sub // tile, k * sub % tile
            g = dot(b, w[part][:, at:at + sub])
            u = dot(b, w[parts // 2 + part][:, at:at + sub])
            if k < subs - 1:
                hid_ref[:, ds((subs * i + k) * sub, sub)] = act(g, u)
            else:
                g_ref[...] = g
                u_ref[...] = u

    gate_up(0, True)

    @pl.loop(1, gu_steps)
    def _(i):
        gate_up(i, False)

    hid_ref[:, (subs * gu_steps - 1) * sub:] = act(g_ref[...], u_ref[...])

    rows = h_ref.shape[0] // 2

    def send(i, mh):
        cols = ds(i * tile, tile)
        part = pl.ds(mh * rows, rows)
        return pltpu.make_async_remote_copy(
            src_ref=ybuf.at[part, cols], dst_ref=y_ref.at[part, cols], send_sem=send_sem.at[i, mh],
            recv_sem=recv_sem.at[i, mh], device_id={'pipe': right}, device_id_type=pl.DeviceIdType.MESH)

    pl.semaphore_wait(barrier, 1)

    @pl.loop(0, down_steps)
    def _(i):
        slot = lax.rem(i + gu_steps, slots)

        @pl.when(i + slots - 1 < down_steps)
        def _():
            start(fetch_down(i + slots - 1, lax.rem(i + gu_steps + slots - 1, slots)))

        for c in fetch_down(i, slot):
            c.wait()
        cols = ds(i * tile, tile)
        for mh in range(2):
            part = slice(mh * rows, (mh + 1) * rows)
            out = h_ref[part, cols].astype(F32)
            for k in range(parts):
                out = out + dot(hid_ref[part, k * depth:(k + 1) * depth], buf[slot, k])
            ybuf[part, cols] = out.astype(BF16)
            send(i, mh).start()

    @pl.loop(0, down_steps)
    def _(i):
        for mh in range(2):
            send(i, mh).wait()


def params(limit_mib, **kwargs):
    return pltpu.CompilerParams(vmem_limit_bytes=limit_mib * MIB, **kwargs)


def solution(mesh):
    stages = mesh.shape['pipe']

    def device_step(x, slice_idx, k_cache, v_cache, w_q, w_kv, w_o, w_gate, w_up, w_down):
        seq, width = x.shape
        cache_len, n_heads, head_dim = k_cache.shape
        pairs = n_heads // 2
        x, w_q, w_kv, w_o, w_gate, w_up, w_down = map(in_hbm, (x, w_q[0], w_kv[0], w_o[0], w_gate[0], w_up[0], w_down[0]))
        ff = w_gate.shape[1]
        k4 = in_hbm(k_cache.reshape(cache_len, pairs, 2, head_dim))
        v4 = in_hbm(v_cache.reshape(cache_len, pairs, 2, head_dim))
        phases = (2, 2, 4)
        gathered = lambda count: [pltpu.VMEM((count, cache_len, 2, head_dim), BF16)] * 2
        big = lambda *shape: pltpu.VMEM(shape, BF16)
        dma = pltpu.SemaphoreType.DMA

        q, kv, kt, vt = pl.pallas_call(
            functools.partial(qkv_kernel, phases[0], seq), name='qkv',
            in_specs=[SMEM, HBM, HBM, HBM, HBM, HBM], out_specs=[VMEM] * 4,
            out_shape=[pltpu.VMEM((seq, width), BF16), pltpu.VMEM((seq, 2 * width), BF16)] + gathered(phases[0]),
            scratch_shapes=[big(seq, width), big(seq, width), big(3, width, 1024), dma, dma((3,)), dma((2,))],
            compiler_params=params(18),
        )(slice_idx, x, w_q, w_kv, k4, v4)

        outs, lses, first = [], [], 0
        for phase, count in enumerate(phases):
            last = phase == len(phases) - 1
            native = (count, 2 * cache_len, head_dim)
            lse_shape = pltpu.VMEM((count, 2, seq), F32)
            mine = big(seq, count * 256)
            if last:
                extra = [lse_shape, big(seq, width), big(2, width, 512), mine, dma((2,)), dma((4,))]
                shapes = [jax.ShapeDtypeStruct((n_heads, seq), F32), big(seq, width), big(seq, width)] + [big(width, 512)] * 4
                more = (*outs, *lses, x, w_o, w_gate, w_up)
            else:
                extra = []
                shapes = [lse_shape, mine] + gathered(phases[phase + 1])
                more = (k4, v4)
            lse, *res = pl.pallas_call(
                functools.partial(attn_kernel, first, 0 if last else phases[phase + 1], len(outs) if last else 0, seq), name='attn',
                in_specs=[SMEM] + [VMEM] * (4 + (2 * len(outs) if last else 0)) + [HBM] * (4 if last else 2), out_specs=[VMEM] * len(shapes), out_shape=shapes,
                scratch_shapes=extra + [pltpu.VMEM((count, 2, 8, QH), F32), pltpu.VMEM((count, 2, 8, QH), F32), pltpu.VMEM((count, 2, 256, QH), F32),
                                        pltpu.VMEM((2, 2 * seq, QH), F32), big(2, 2 * seq, QH),
                                        pltpu.VMEM((2, 8, QH), F32), pltpu.VMEM((2, 8, QH), F32), dma((2,))],
                compiler_params=params(17 if last else 9),
            )(slice_idx, q, kv, kt.reshape(native), vt.reshape(native), *more)
            lses.append(lse)
            first += count
            if last:
                h, b, *gu_first = res
            else:
                o, kt, vt = res
                outs.append(o)
        y_next = pl.pallas_call(
            functools.partial(mlp_kernel, stages), name='mlp', in_specs=[VMEM] * 6 + [HBM] * 3, out_specs=HBM,
            out_shape=jax.ShapeDtypeStruct((seq, width), BF16),
            scratch_shapes=[big(seq, ff), big(2, 4, width, 512), pltpu.VMEM((seq, 256), F32), pltpu.VMEM((seq, 256), F32), big(seq, width),
                            dma((2, 4)), dma((4, 2)), dma((4, 2))],
            compiler_params=params(34, collective_id=0, has_side_effects=True),
        )(h, b, *gu_first, w_gate, w_up, w_down)
        return y_next, lse.T

    rows_spec = P(('data', 'pipe'), None)
    cache_spec = P(('data', 'pipe'), None, None)
    stage_spec = P('pipe', None, None)
    return jax.shard_map(
        device_step,
        mesh=mesh,
        in_specs=(rows_spec, P(('data', 'pipe')), cache_spec, cache_spec) + (stage_spec,) * 6,
        out_specs=(rows_spec, rows_spec),
        check_vma=False,
    )
```
